512 devices in a mesh: ctx: 32 (over y, x), tp: 16 (over z, core).
Axes of the slice: x: 4, y: 8, z: 8, core: 2. Of those that a mesh axis runs over, the one named last changes fastest.
Arguments:
- queries: bfloat16 [8192, 8192], P('ctx', 'tp'), may hold values from -8 to 8
- keys: bfloat16 [8192, 1024], P('ctx'), may hold values from -6 to 6
- values: bfloat16 [8192, 1024], P('ctx'), may hold values from -6 to 6
Outputs:
- attended: bfloat16 [8192, 8192], P('ctx', 'tp')
The draws below stay inside these ranges and needn't reach their ends.
All inputs are finite; a program needn't handle non-finite values.
Results may differ from the reference program's by a relative error of at most 0.0032.
Values may be sent and summed in bfloat16 or wider, within the bound.
No kernel may reach another device: no remote copies, remote signals or barrier semaphores. Data moves between devices by JAX's collectives and lax.ppermute only.
A program may use at most 64 MiB of HBM per device.

```python
import jax
import jax.numpy as jnp
from jax import lax

HEADS = 64
KV_HEADS = 8
HEAD_DIM = 128
TOKENS = 8192


def draw_keys(key, part):
    drawn = jnp.clip(jax.random.normal(jax.random.fold_in(key, 11), (TOKENS, KV_HEADS * HEAD_DIM), jnp.float32), -6.0, 6.0)
    return drawn.astype(jnp.bfloat16)


def draw_queries(key, part):
    drawn = jnp.clip(2.5 * jax.random.normal(jax.random.fold_in(key, 13), (TOKENS, HEADS * HEAD_DIM), jnp.float32), -8.0, 8.0)
    return drawn.astype(jnp.bfloat16)


def block_levels(stream_key, dims, pieces, least, high):
    factor_of, own = 1.0, jax.random.fold_in(stream_key, 6)
    for dim, blocks in pieces:
        draws = jnp.exp(jax.random.uniform(jax.random.fold_in(own, dim), (blocks,), jnp.float32, least / len(pieces), high / len(pieces)))
        factor_of = factor_of * jnp.repeat(draws, dims[dim] // blocks).reshape([-1 if axis == dim else 1 for axis in range(len(dims))])
    return factor_of


def gaussian(rng, extent, width, most, pieces=(), held_as=jnp.bfloat16):
    entries = jax.random.normal(rng, extent, jnp.float32) * width
    if len(pieces) > 0:
        entries = block_levels(rng, extent, pieces, -0.22, 0.18) * entries
    return jnp.clip(entries, min=-most, max=most).astype(held_as)


def setup_inputs(seed: int = 0) -> dict:
    splits = jax.random.split(jax.random.key(seed), 4)
    return {
        "queries": draw_queries(jax.random.fold_in(splits[3], 71), 0),
        "keys": draw_keys(jax.random.fold_in(splits[3], 71), 0),
        "values": gaussian(splits[2], (TOKENS, KV_HEADS * HEAD_DIM), 1.0, 6.0, ((0, 32),)),
    }


def attention(queries, keys, values):
    group_size = HEADS // KV_HEADS
    score_scale = HEAD_DIM ** -0.5
    token_positions = jnp.arange(TOKENS, dtype=jnp.int32)
    allowed = token_positions[None, :] <= token_positions[:, None]

    def one_head(head_index):
        kv_index = head_index // group_size
        query_head = lax.dynamic_slice_in_dim(queries, head_index * HEAD_DIM, HEAD_DIM, 1)
        key_head = lax.dynamic_slice_in_dim(keys, kv_index * HEAD_DIM, HEAD_DIM, 1)
        value_head = lax.dynamic_slice_in_dim(values, kv_index * HEAD_DIM, HEAD_DIM, 1)
        scores = jnp.dot(query_head, key_head.T, preferred_element_type=jnp.float32) * score_scale
        scores = jnp.where(allowed, scores, -jnp.inf)
        row_peak = jnp.max(scores, axis=1, keepdims=True)
        raw_weights = jnp.where(allowed, jnp.exp(scores - row_peak), 0.0)
        row_total = jnp.sum(raw_weights, axis=1, keepdims=True)
        weights = raw_weights.astype(jnp.bfloat16)
        summed = jnp.dot(weights, value_head, preferred_element_type=jnp.float32)
        return (summed / row_total).astype(jnp.bfloat16)

    per_head = lax.map(one_head, jnp.arange(HEADS, dtype=jnp.int32))
    return jnp.transpose(per_head, (1, 0, 2)).reshape(TOKENS, HEADS * HEAD_DIM)


def reference(queries, keys, values):
    return attention(queries, keys, values)
```

```python
import functools

import jax
import jax.numpy as jnp
from jax import lax
from jax.experimental import pallas as pl
from jax.experimental.pallas import tpu as pltpu
from jax.sharding import PartitionSpec as P

HEADS = 64
KV_HEADS = 8
HEAD_DIM = 128
GROUP = HEADS // KV_HEADS
Y, X, Z, C = 8, 4, 8, 2
LOW = -1e30
EXPONENT = HEAD_DIM**-0.5 * 1.4426950408889634


def place(y, x, z, c):
    return (((y % Y) * X + (x % X)) * Z + z) * C + c


def move(a, first, second):
    pairs = [
        (place(y, x, z, c), place(y + by[0], x + by[1], z, c))
        for y in range(Y)
        for x in range(X)
        for z in range(Z)
        for c, by in enumerate((first, second))
    ]
    return lax.ppermute(a, ("ctx", "tp"), pairs)


def swap(a):
    return lax.ppermute(a, "tp", [(i, i ^ 1) for i in range(Z * C)])


def absorb(q_ref, kv, state, heads, limit=None):
    acc_ref, peak_ref, total_ref = state
    keys = kv[:, :HEAD_DIM]
    values_t = kv[:, HEAD_DIM:].T
    rows = q_ref.shape[0]
    for h in range(heads):
        q = q_ref[:, h * HEAD_DIM : (h + 1) * HEAD_DIM]
        scores = lax.dot_general(keys, q, (((1,), (1,)), ((), ())), preferred_element_type=jnp.float32)
        if limit is not None:
            at_key = lax.broadcasted_iota(jnp.int32, scores.shape, 0)
            at_query = lax.broadcasted_iota(jnp.int32, scores.shape, 1)
            scores = jnp.where(at_key <= at_query, scores, LOW)
        old_peak = peak_ref[h : h + 1, :]
        peak = jnp.maximum(old_peak, jnp.max(scores, axis=0, keepdims=True))
        weights = jnp.exp2((scores - peak) * EXPONENT)
        shrink = jnp.exp2((old_peak - peak) * EXPONENT)
        total_ref[h : h + 1, :] = total_ref[h : h + 1, :] * shrink + jnp.sum(weights, axis=0, keepdims=True)
        peak_ref[h : h + 1, :] = peak
        acc_ref[h] = acc_ref[h] * shrink + jnp.dot(
            values_t, weights.astype(jnp.bfloat16), preferred_element_type=jnp.float32
        )


def start_kernel(flags, q_ref, own_ref, near_ref, far_a_ref, far_b_ref, acc_ref, peak_ref, total_ref):
    state = (acc_ref, peak_ref, total_ref)
    acc_ref[...] = jnp.zeros_like(acc_ref)
    peak_ref[...] = jnp.full_like(peak_ref, LOW)
    total_ref[...] = jnp.zeros_like(total_ref)

    @pl.when(flags[0] == 1)
    def _():
        absorb(q_ref, own_ref[...], state, GROUP, limit=True)

    @pl.when(flags[1] == 1)
    def _():
        absorb(q_ref, near_ref[...], state, GROUP)

    @pl.when(flags[2] == 1)
    def _():
        absorb(q_ref, jnp.concatenate([far_a_ref[...], far_b_ref[...]], 0), state, GROUP)


def step_kernel(flags, q_ref, a_ref, b_ref, acc_in, peak_in, total_in, acc_ref, peak_ref, total_ref):
    peak_ref[...] = peak_in[...]
    total_ref[...] = total_in[...]
    acc_ref[...] = acc_in[...]

    @pl.when(flags[0] == 1)
    def _():
        absorb(q_ref, jnp.concatenate([a_ref[...], b_ref[...]], 0), (acc_ref, peak_ref, total_ref), GROUP)


def merge_kernel(acc_ref, peak_ref, total_ref, acc2_ref, stat2_ref, out_ref):
    for h in range(GROUP // 2):
        peak, peak2 = peak_ref[h : h + 1, :], stat2_ref[h : h + 1, :]
        top = jnp.maximum(peak, peak2)
        w = jnp.exp2((peak - top) * EXPONENT)
        w2 = jnp.exp2((peak2 - top) * EXPONENT)
        total = total_ref[h : h + 1, :] * w + stat2_ref[GROUP // 2 + h : GROUP // 2 + h + 1, :] * w2
        normed = (acc_ref[h] * w + acc2_ref[h] * w2) / total
        out_ref[:, h * HEAD_DIM : (h + 1) * HEAD_DIM] = normed.T.astype(jnp.bfloat16)


VMEM = pl.BlockSpec(memory_space=pltpu.VMEM)
LIMIT = pltpu.CompilerParams(vmem_limit_bytes=24 * 2**20)
SMEM = pl.BlockSpec(memory_space=pltpu.SMEM)


def state_shapes(rows):
    return (
        jax.ShapeDtypeStruct((GROUP, HEAD_DIM, rows), jnp.float32),
        jax.ShapeDtypeStruct((GROUP, rows), jnp.float32),
        jax.ShapeDtypeStruct((GROUP, rows), jnp.float32),
    )


def cost(rows, keys):
    return pl.CostEstimate(
        flops=4 * rows * GROUP * keys * HEAD_DIM,
        bytes_accessed=4 * keys * HEAD_DIM + 2 * rows * GROUP * HEAD_DIM,
        transcendentals=rows * GROUP * keys,
    )


def begin(flags, q, own, near, far_a, far_b):
    rows = q.shape[0]
    return pl.pallas_call(
        start_kernel,
        out_shape=state_shapes(rows),
        in_specs=[SMEM] + [VMEM] * 5,
        out_specs=(VMEM,) * 3,
        cost_estimate=cost(rows, 512),
        compiler_params=LIMIT,
        name="own_row",
    )(flags, q, own, near, far_a, far_b)


def step(flags, q, a, b, state):
    rows = q.shape[0]
    return pl.pallas_call(
        step_kernel,
        out_shape=state_shapes(rows),
        in_specs=[SMEM] + [VMEM] * 6,
        out_specs=(VMEM,) * 3,
        input_output_aliases={4: 0, 5: 1, 6: 2},
        cost_estimate=cost(rows, a.shape[0] + b.shape[0]),
        compiler_params=LIMIT,
        name="other_row",
    )(flags, q, a, b, *state)


def merge(state, acc2, stat2):
    rows = acc2.shape[2]
    return pl.pallas_call(
        merge_kernel,
        out_shape=jax.ShapeDtypeStruct((rows, GROUP // 2 * HEAD_DIM), jnp.bfloat16),
        in_specs=[VMEM] * 5,
        out_specs=VMEM,
        cost_estimate=pl.CostEstimate(flops=rows * HEAD_DIM * 32, bytes_accessed=rows * HEAD_DIM * 32, transcendentals=0),
        compiler_params=LIMIT,
        name="merge",
    )(*state, acc2, stat2)


def shards(queries, keys, values):
    ctx, tp = lax.axis_index("ctx"), lax.axis_index("tp")
    y, x, core = ctx // X, ctx % X, tp % C
    half = queries.shape[0] // 2
    column = tp // C * HEAD_DIM
    own = jnp.concatenate(
        [lax.dynamic_slice_in_dim(a, column, HEAD_DIM, 1) for a in (keys, values)], 1
    )
    mine = lax.dynamic_slice_in_dim(own, core * half, half, 0)
    others = lax.dynamic_slice_in_dim(own, (1 - core) * half, half, 0)
    near = move(own, (0, 1), (0, -1))
    far_a = move(mine, (0, 2), (0, -2))
    q = jnp.concatenate([queries, swap(queries)], 1)
    swapped = swap(jnp.concatenate([near, far_a], 0))
    far_b = swapped[2 * half :]

    a = jnp.concatenate([near, mine, others], 0)
    b = jnp.concatenate([far_a, far_b, swapped[: 2 * half]], 0)

    flag = lambda *tests: jnp.stack([jnp.asarray(t).astype(jnp.int32) for t in tests])
    near_x = (x + jnp.where(core == 0, X - 1, 1)) % X
    state = begin(
        flag(core == 0, near_x < x, (core == 1) & (x >= 2)), q, own, near, far_a, far_b
    )
    for n in range(1, 5):
        if n == 4:
            a, b = a[: 3 * half], b[:half]
        a = move(a, (1, 0), (-1, 0))
        b = move(b, (1, 0), (-1, 0))
        state = step(flag(jnp.where(core == 0, y >= n, y + n >= Y)), q, a, b, state)
    acc, peak, total = state
    g = GROUP // 2
    acc2 = swap(acc[g:])
    stat2 = swap(jnp.concatenate([peak[g:], total[g:]], 0))
    return merge(state, acc2, stat2)


def solution(mesh):
    in_specs = (P("ctx", "tp"), P("ctx", None), P("ctx", None))
    return jax.shard_map(shards, mesh=mesh, in_specs=in_specs, out_specs=P("ctx", "tp"), check_vma=False)
```

```python
import functools

import jax
import jax.numpy as jnp
from jax import lax
from jax.experimental import pallas as pl
from jax.experimental.pallas import tpu as pltpu
from jax.sharding import PartitionSpec as P

HEADS = 64
KV_HEADS = 8
HEAD_DIM = 128
GROUP = HEADS // KV_HEADS
Y, X, Z, C = 8, 4, 8, 2
MASKED, EMPTY = -1e30, -1e29
EXPONENT = HEAD_DIM**-0.5 * 1.4426950408889634
PEAK, TOTAL, ROWS = HEAD_DIM, HEAD_DIM + 1, HEAD_DIM + 8


def place(y, x, z, c):
    return (((y % Y) * X + (x % X)) * Z + z) * C + c


def move(a, first, second):
    pairs = [
        (place(y, x, z, c), place(y, x + by, z, c))
        for y in range(Y)
        for x in range(X)
        for z in range(Z)
        for c, by in enumerate((first, second))
    ]
    return lax.ppermute(a, ("ctx", "tp"), pairs)


def swap(a):
    return lax.ppermute(a, "tp", [(i, i ^ 1) for i in range(Z * C)])


def absorb(q_ref, kv_refs, read, write, scores_ref, weights_ref, values_ref, delta=None):
    sub = 256 if delta is None else 128
    parts = []
    for ref in kv_refs:
        parts += [(ref, at) for at in range(0, ref.shape[0], sub)]
    count = len(parts) * sub
    for n, (ref, at) in enumerate(parts):
        values_ref[:, n * sub : (n + 1) * sub] = ref[at : at + sub, HEAD_DIM:].T
    rows = q_ref.shape[0]
    if delta is not None:
        ahead = lax.broadcasted_iota(jnp.int32, (sub, rows), 0) - lax.broadcasted_iota(jnp.int32, (sub, rows), 1)

    def score(h):
        q = q_ref[:, h * HEAD_DIM : (h + 1) * HEAD_DIM]
        top = None
        for n, (ref, at) in enumerate(parts):
            s = lax.dot_general(
                ref[at : at + sub, :HEAD_DIM], q, (((1,), (1,)), ((), ())), preferred_element_type=jnp.float32
            )
            if delta is not None:
                s = jnp.where(ahead <= -(delta + n * (X * rows)), s, MASKED)
            scores_ref[h % 2, n * sub : (n + 1) * sub, :] = s
            t = jnp.max(s.reshape(sub // 8, 8, rows), axis=0)
            top = t if top is None else jnp.maximum(top, t)
        return jnp.max(top, axis=0, keepdims=True)

    def weigh(h, top):
        old_peak = read(h, PEAK)
        peak = jnp.maximum(old_peak, top)
        shrink = jnp.exp2((old_peak - peak) * EXPONENT)
        total = None
        for n in range(len(parts)):
            w = jnp.exp2((scores_ref[h % 2, n * sub : (n + 1) * sub, :] - peak) * EXPONENT)
            t = jnp.sum(w.reshape(sub // 8, 8, rows), axis=0)
            total = t if total is None else total + t
            weights_ref[h % 2, n * sub : (n + 1) * sub, :] = w.astype(jnp.bfloat16)
        write(h, TOTAL, read(h, TOTAL) * shrink + jnp.sum(total, axis=0, keepdims=True))
        write(h, PEAK, peak)
        return shrink

    def combine(h, shrink):
        add = jnp.dot(values_ref[:, :count], weights_ref[h % 2, :count, :], preferred_element_type=jnp.float32)
        write(h, None, read(h, None) * shrink + add)

    top, shrink = {0: score(0)}, {}
    for h in range(GROUP + 1):
        if h + 1 < GROUP:
            top[h + 1] = score(h + 1)
        if h >= 1:
            combine(h - 1, shrink[h - 1])
        if h < GROUP:
            shrink[h] = weigh(h, top[h])


def at_row(ref, h, row):
    return ref.at[h, :HEAD_DIM] if row is None else ref.at[h, row : row + 1]


def kernel(n_kv, first, last, *refs):
    flags, q_ref = refs[:2]
    kv_refs = refs[2 : 2 + n_kv]
    n = 2 + n_kv
    if not first:
        state_in = refs[n]
        n += 1
    outs = refs[n : n + 1 + last]
    scratch = refs[n + 1 + last :]
    if first:

        def read(h, row):
            shape = (HEAD_DIM if row is None else 1, q_ref.shape[0])
            return jnp.full(shape, EMPTY if row == PEAK else 0.0, jnp.float32)
    else:

        def read(h, row):
            return at_row(state_in, h, row)[...]

    def target(h):
        per = GROUP // len(outs)
        return outs[h // per], h % per

    def write(h, row, value):
        ref, k = target(h)
        at_row(ref, k, row)[...] = value

    @pl.when(flags[0] == 0)
    def _():
        for h in range(GROUP):
            for row in (None, PEAK, TOTAL):
                write(h, row, read(h, row))

    @pl.when(flags[0] == 1)
    def _():
        absorb(q_ref, kv_refs, read, write, *scratch)

    @pl.when(flags[0] == 2)
    def _():
        absorb(q_ref, kv_refs, read, write, *scratch, delta=flags[1])


def merge_kernel(mine_ref, theirs_ref, out_ref):
    for h in range(GROUP // 2):
        peak, peak2 = mine_ref[h, PEAK : PEAK + 1], theirs_ref[h, PEAK : PEAK + 1]
        top = jnp.maximum(peak, peak2)
        w = jnp.exp2((peak - top) * EXPONENT)
        w2 = jnp.exp2((peak2 - top) * EXPONENT)
        total = mine_ref[h, TOTAL : TOTAL + 1] * w + theirs_ref[h, TOTAL : TOTAL + 1] * w2
        normed = (mine_ref[h, :HEAD_DIM] * w + theirs_ref[h, :HEAD_DIM] * w2) / total
        out_ref[:, h * HEAD_DIM : (h + 1) * HEAD_DIM] = normed.T.astype(jnp.bfloat16)


VMEM = pl.BlockSpec(memory_space=pltpu.VMEM)
SMEM = pl.BlockSpec(memory_space=pltpu.SMEM)
LIMIT = pltpu.CompilerParams(vmem_limit_bytes=24 * 2**20)


def run(name, flags, q, kvs, state=None, last=False):
    rows = q.shape[0]
    keys = sum(kv.shape[0] for kv in kvs)
    first = state is None
    heads = GROUP // (1 + last)
    shape = tuple(pltpu.VMEM((heads, ROWS, rows), jnp.float32) for _ in range(1 + last))
    return pl.pallas_call(
        functools.partial(kernel, len(kvs), first, last),
        out_shape=shape if last else shape[0],
        in_specs=[SMEM] + [VMEM] * (1 + len(kvs) + (not first)),
        out_specs=(VMEM,) * 2 if last else VMEM,
        input_output_aliases={} if first or last else {2 + len(kvs): 0},
        scratch_shapes=[
            pltpu.VMEM((2, keys, rows), jnp.float32),
            pltpu.VMEM((2, keys, rows), jnp.bfloat16),
            pltpu.VMEM((HEAD_DIM, keys), jnp.bfloat16),
        ],
        cost_estimate=pl.CostEstimate(
            flops=4 * rows * GROUP * keys * HEAD_DIM,
            bytes_accessed=4 * keys * HEAD_DIM + 2 * rows * GROUP * HEAD_DIM,
            transcendentals=rows * GROUP * keys,
        ),
        compiler_params=LIMIT,
        name=name,
    )(flags, q, *kvs, *(() if first else (state,)))


def merge(mine, theirs):
    rows = mine.shape[2]
    return pl.pallas_call(
        merge_kernel,
        out_shape=jax.ShapeDtypeStruct((rows, GROUP // 2 * HEAD_DIM), jnp.bfloat16),
        in_specs=[VMEM] * 2,
        out_specs=VMEM,
        cost_estimate=pl.CostEstimate(flops=rows * HEAD_DIM * 32, bytes_accessed=rows * HEAD_DIM * 32, transcendentals=0),
        compiler_params=LIMIT,
        name="merge",
    )(mine, theirs)


def shards(queries, keys, values):
    ctx, tp = lax.axis_index("ctx"), lax.axis_index("tp")
    y, x, core = ctx // X, ctx % X, tp % C
    rows = queries.shape[0]
    half = rows // 2
    column = tp // C * HEAD_DIM
    mine = jnp.concatenate(
        [lax.dynamic_slice(a, (core * half, column), (half, HEAD_DIM)) for a in (keys, values)], 1
    )
    by_row = lax.all_to_all(
        jnp.broadcast_to(mine[None], (Y,) + mine.shape), "ctx", 0, 0,
        axis_index_groups=[[b * X + a for b in range(Y)] for a in range(X)],
    ).reshape(Y * half, 2 * HEAD_DIM)
    low, high = by_row[: Y * half // 2], by_row[Y * half // 2 :]
    one_low, one_high = move(low, 1, -1), move(high, 1, -1)
    q = jnp.concatenate([queries, swap(queries)], 1)
    other = move(by_row, -1, 1)
    two_low, two_high = move(one_low, 1, -1), move(one_high, 1, -1)

    def flags(shift, first_row, n_rows):
        from_x = (x + shift) % X
        delta = ((first_row - y) * X + from_x - x) * rows + core * half
        none, every = delta >= rows, delta + (n_rows - 1) * X * rows + half - 1 <= 0
        return jnp.stack([jnp.where(none, 0, jnp.where(every, 1, 2)), delta]).astype(jnp.int32)

    toward = jnp.where(core == 0, -1, 1)
    state = run("own_column", flags(0, 0, Y), q, [by_row])
    state = run("next_column", flags(toward, 0, Y), q, [one_low, one_high], state)
    state = run("other_column", flags(-toward, 0, Y), q, [other], state)
    state = run("far_low", flags(2, 0, Y // 2), q, [two_low], state)
    mine, theirs = run("far_high", flags(2, Y // 2, Y // 2), q, [two_high], state, last=True)
    return merge(mine, swap(theirs))


def solution(mesh):
    in_specs = (P("ctx", "tp"), P("ctx", None), P("ctx", None))
    return jax.shard_map(shards, mesh=mesh, in_specs=in_specs, out_specs=P("ctx", "tp"), check_vma=False)
```

```python
import functools

import jax
import jax.numpy as jnp
from jax import lax
from jax.experimental import pallas as pl
from jax.experimental.pallas import tpu as pltpu
from jax.sharding import PartitionSpec as P

HEADS = 64
KV_HEADS = 8
HEAD_DIM = 128
GROUP = HEADS // KV_HEADS
Y, X, Z, C = 8, 4, 8, 2
MASKED, EMPTY = -1e30, -1e29
EXPONENT = HEAD_DIM**-0.5 * 1.4426950408889634
PEAK, TOTAL, ROWS = HEAD_DIM, HEAD_DIM + 1, HEAD_DIM + 8


def place(y, x, z, c):
    return (((y % Y) * X + (x % X)) * Z + z) * C + c


def move(a, first, second):
    pairs = [
        (place(y, x, z, c), place(y, x + by, z, c))
        for y in range(Y)
        for x in range(X)
        for z in range(Z)
        for c, by in enumerate((first, second))
    ]
    return lax.ppermute(a, ("ctx", "tp"), pairs)


def swap(a):
    return lax.ppermute(a, "tp", [(i, i ^ 1) for i in range(Z * C)])


def absorb(q_ref, kv_refs, read, write, scores_ref, weights_ref, values_ref, delta=None):
    sub = 256 if delta is None else 128
    parts = []
    for ref in kv_refs:
        parts += [(ref, at) for at in range(0, ref.shape[0], sub)]
    count = len(parts) * sub
    for n, (ref, at) in enumerate(parts):
        values_ref[:, n * sub : (n + 1) * sub] = ref[at : at + sub, HEAD_DIM:].T
    rows = q_ref.shape[0]
    if delta is not None:
        ahead = lax.broadcasted_iota(jnp.int32, (sub, rows), 0) - lax.broadcasted_iota(jnp.int32, (sub, rows), 1)

    def score(h):
        q = q_ref[:, h * HEAD_DIM : (h + 1) * HEAD_DIM]
        top = None
        for n, (ref, at) in enumerate(parts):
            s = lax.dot_general(
                ref[at : at + sub, :HEAD_DIM], q, (((1,), (1,)), ((), ())), preferred_element_type=jnp.float32
            )
            if delta is not None:
                s = jnp.where(ahead <= -(delta + n * (X * rows)), s, MASKED)
            scores_ref[h % 2, n * sub : (n + 1) * sub, :] = s
            t = jnp.max(s.reshape(sub // 8, 8, rows), axis=0)
            top = t if top is None else jnp.maximum(top, t)
        return jnp.max(top, axis=0, keepdims=True)

    def weigh(h, top):
        old_peak = read(h, PEAK)
        peak = jnp.maximum(old_peak, top)
        shrink = jnp.exp2((old_peak - peak) * EXPONENT)
        total = None
        for n in range(len(parts)):
            w = jnp.exp2((scores_ref[h % 2, n * sub : (n + 1) * sub, :] - peak) * EXPONENT)
            t = jnp.sum(w.reshape(sub // 8, 8, rows), axis=0)
            total = t if total is None else total + t
            weights_ref[h % 2, n * sub : (n + 1) * sub, :] = w.astype(jnp.bfloat16)
        write(h, TOTAL, read(h, TOTAL) * shrink + jnp.sum(total, axis=0, keepdims=True))
        write(h, PEAK, peak)
        return shrink

    def combine(h, shrink):
        add = jnp.dot(values_ref[:, :count], weights_ref[h % 2, :count, :], preferred_element_type=jnp.float32)
        write(h, None, read(h, None) * shrink + add)

    top, shrink = {0: score(0)}, {}
    for h in range(GROUP + 1):
        if h + 1 < GROUP:
            top[h + 1] = score(h + 1)
        if h >= 1:
            combine(h - 1, shrink[h - 1])
        if h < GROUP:
            shrink[h] = weigh(h, top[h])


def at_row(ref, h, row):
    return ref.at[h, :HEAD_DIM] if row is None else ref.at[h, row : row + 1]


def kernel(n_kv, first, last, *refs):
    flags, q_ref = refs[:2]
    kv_refs = refs[2 : 2 + n_kv]
    n = 2 + n_kv
    if not first:
        state_in = refs[n]
        n += 1
    outs = refs[n : n + 1 + last]
    scratch = refs[n + 1 + last :]
    if first:

        def read(h, row):
            shape = (HEAD_DIM if row is None else 1, q_ref.shape[0])
            return jnp.full(shape, EMPTY if row == PEAK else 0.0, jnp.float32)
    else:

        def read(h, row):
            return at_row(state_in, h, row)[...]

    def target(h):
        per = GROUP // len(outs)
        return outs[h // per], h % per

    def write(h, row, value):
        ref, k = target(h)
        at_row(ref, k, row)[...] = value

    @pl.when(flags[0] == 0)
    def _():
        for h in range(GROUP):
            for row in (None, PEAK, TOTAL):
                write(h, row, read(h, row))

    @pl.when(flags[0] == 1)
    def _():
        absorb(q_ref, kv_refs, read, write, *scratch)

    @pl.when(flags[0] == 2)
    def _():
        absorb(q_ref, kv_refs, read, write, *scratch, delta=flags[1])


def merge_kernel(mine_ref, theirs_ref, out_ref):
    for h in range(GROUP // 2):
        peak, peak2 = mine_ref[h, PEAK : PEAK + 1], theirs_ref[h, PEAK : PEAK + 1]
        top = jnp.maximum(peak, peak2)
        w = jnp.exp2((peak - top) * EXPONENT)
        w2 = jnp.exp2((peak2 - top) * EXPONENT)
        total = mine_ref[h, TOTAL : TOTAL + 1] * w + theirs_ref[h, TOTAL : TOTAL + 1] * w2
        normed = (mine_ref[h, :HEAD_DIM] * w + theirs_ref[h, :HEAD_DIM] * w2) / total
        out_ref[:, h * HEAD_DIM : (h + 1) * HEAD_DIM] = normed.T.astype(jnp.bfloat16)


VMEM = pl.BlockSpec(memory_space=pltpu.VMEM)
SMEM = pl.BlockSpec(memory_space=pltpu.SMEM)
LIMIT = pltpu.CompilerParams(vmem_limit_bytes=24 * 2**20)


def run(name, flags, q, kvs, state=None, last=False):
    rows = q.shape[0]
    keys = sum(kv.shape[0] for kv in kvs)
    first = state is None
    heads = GROUP // (1 + last)
    shape = tuple(pltpu.VMEM((heads, ROWS, rows), jnp.float32) for _ in range(1 + last))
    return pl.pallas_call(
        functools.partial(kernel, len(kvs), first, last),
        out_shape=shape if last else shape[0],
        in_specs=[SMEM] + [VMEM] * (1 + len(kvs) + (not first)),
        out_specs=(VMEM,) * 2 if last else VMEM,
        input_output_aliases={} if first or last else {2 + len(kvs): 0},
        scratch_shapes=[
            pltpu.VMEM((2, keys, rows), jnp.float32),
            pltpu.VMEM((2, keys, rows), jnp.bfloat16),
            pltpu.VMEM((HEAD_DIM, keys), jnp.bfloat16),
        ],
        cost_estimate=pl.CostEstimate(
            flops=4 * rows * GROUP * keys * HEAD_DIM,
            bytes_accessed=4 * keys * HEAD_DIM + 2 * rows * GROUP * HEAD_DIM,
            transcendentals=rows * GROUP * keys,
        ),
        compiler_params=LIMIT,
        name=name,
    )(flags, q, *kvs, *(() if first else (state,)))


def spread_kernel(place_ref, keys_ref, values_ref, out_ref):
    both = jnp.concatenate([keys_ref[...], values_ref[...]], 1)
    for n in range(out_ref.shape[0]):
        out_ref[n] = both


def spread(place_of, keys, values, half):
    block = pl.BlockSpec((half, HEAD_DIM), lambda n, at: (at[0], at[1]))
    return pl.pallas_call(
        spread_kernel,
        grid_spec=pltpu.PrefetchScalarGridSpec(
            num_scalar_prefetch=1,
            grid=(1,),
            in_specs=[block, block],
            out_specs=pl.BlockSpec((Y, half, 2 * HEAD_DIM), lambda n, at: (0, 0, 0)),
        ),
        out_shape=jax.ShapeDtypeStruct((Y, half, 2 * HEAD_DIM), jnp.bfloat16),
        compiler_params=LIMIT,
        name="spread",
    )(place_of, *(pltpu.with_memory_space_constraint(a, pltpu.HBM) for a in (keys, values)))


def merge(mine, theirs):
    rows = mine.shape[2]
    return pl.pallas_call(
        merge_kernel,
        out_shape=jax.ShapeDtypeStruct((rows, GROUP // 2 * HEAD_DIM), jnp.bfloat16),
        in_specs=[VMEM] * 2,
        out_specs=VMEM,
        cost_estimate=pl.CostEstimate(flops=rows * HEAD_DIM * 32, bytes_accessed=rows * HEAD_DIM * 32, transcendentals=0),
        compiler_params=LIMIT,
        name="merge",
    )(mine, theirs)


def shards(queries, keys, values):
    ctx, tp = lax.axis_index("ctx"), lax.axis_index("tp")
    y, x, core = ctx // X, ctx % X, tp % C
    rows = queries.shape[0]
    half = rows // 2
    column = tp // C * HEAD_DIM
    copies = spread(jnp.stack([core, tp // C]).astype(jnp.int32), keys, values, half)
    by_row = lax.all_to_all(
        copies, "ctx", 0, 0, axis_index_groups=[[b * X + a for b in range(Y)] for a in range(X)]
    ).reshape(Y * half, 2 * HEAD_DIM)
    one = move(by_row, 1, -1)
    q = jnp.concatenate([queries, swap(queries)], 1)

    def flags(shift, first_row, n_rows):
        from_x = (x + shift) % X
        delta = ((first_row - y) * X + from_x - x) * rows + core * half
        none, every = delta >= rows, delta + (n_rows - 1) * X * rows + half - 1 <= 0
        return jnp.stack([jnp.where(none, 0, jnp.where(every, 1, 2)), delta]).astype(jnp.int32)

    toward = jnp.where(core == 0, -1, 1)
    state = run("own_column", flags(0, 0, Y), q, [by_row])
    by_row, state = lax.optimization_barrier((by_row, state))
    other = move(by_row, -1, 1)
    two = move(one, 1, -1)
    state = run("next_column", flags(toward, 0, Y), q, [one], state)
    state = run("other_column", flags(-toward, 0, Y), q, [other], state)
    mine, theirs = run("far_column", flags(2, 0, Y), q, [two], state, last=True)
    return merge(mine, swap(theirs))


def solution(mesh):
    in_specs = (P("ctx", "tp"), P("ctx", None), P("ctx", None))
    return jax.shard_map(shards, mesh=mesh, in_specs=in_specs, out_specs=P("ctx", "tp"), check_vma=False)
```

```python
import functools

import jax
import jax.numpy as jnp
from jax import lax
from jax.experimental import pallas as pl
from jax.experimental.pallas import tpu as pltpu
from jax.sharding import PartitionSpec as P


HEADS = 64
KV_HEADS = 8
HEAD_DIM = 128
GROUP = HEADS // KV_HEADS
Y, X, Z, C = 8, 4, 8, 2
MASKED, EMPTY = -1e30, -1e29
EXPONENT = HEAD_DIM**-0.5 * 1.4426950408889634
TOTAL, PEAK, ROWS = HEAD_DIM, HEAD_DIM + 8, HEAD_DIM + 16


def place(y, x, z, c):
    return (((y % Y) * X + (x % X)) * Z + z) * C + c


def move(a, first, second):
    pairs = [
        (place(y, x, z, c), place(y, x + by, z, c))
        for y in range(Y)
        for x in range(X)
        for z in range(Z)
        for c, by in enumerate((first, second))
    ]
    return lax.ppermute(a, ("ctx", "tp"), pairs)


def swap(a):
    return lax.ppermute(a, "tp", [(i, i ^ 1) for i in range(Z * C)])


def absorb(q_ref, kv_ref, count, delta, head_at, heads, state_in, outs, scores_ref, weights_ref, values_ref):
    rows = q_ref.shape[0]
    half = rows // 2
    values_ref[HEAD_DIM:, :count] = jnp.ones((values_ref.shape[0] - HEAD_DIM, count), jnp.bfloat16)
    for at in range(0, count, rows):
        values_ref[:HEAD_DIM, at : at + rows] = kv_ref[at : at + rows, HEAD_DIM:].T
    ahead = lax.broadcasted_iota(jnp.int32, (half, rows), 0) - lax.broadcasted_iota(jnp.int32, (half, rows), 1)
    per = heads // len(outs)
    first_masked = 0 if count < kv_ref.shape[0] else count // half // 2

    def score(h):
        q = q_ref[:, (head_at + h) * HEAD_DIM : (head_at + h + 1) * HEAD_DIM]
        top = None
        for n in range(count // half):
            at = slice(n * half, (n + 1) * half)
            s = lax.dot_general(
                kv_ref[at, :HEAD_DIM], q, (((1,), (1,)), ((), ())), preferred_element_type=jnp.float32
            )
            if n >= first_masked:
                s = jnp.where(ahead <= -(delta + n * (X * rows)), s, MASKED)
            scores_ref[h % 2, at, :] = s
            t = jnp.max(s.reshape(half // 8, 8, rows), axis=0)
            top = t if top is None else jnp.maximum(top, t)
        return jnp.broadcast_to(jnp.max(top, axis=0, keepdims=True), (8, rows))

    def weigh(h, top):
        old_peak = jnp.full((8, rows), EMPTY, jnp.float32) if state_in is None else state_in[h, PEAK:]
        peak = jnp.maximum(old_peak, top)
        for n in range(count // half):
            at = slice(n * half, (n + 1) * half)
            s = scores_ref[h % 2, at, :].reshape(half // 8, 8, rows)
            w = jnp.exp2((s - peak[None]) * EXPONENT)
            weights_ref[h % 2, at, :] = w.reshape(half, rows).astype(jnp.bfloat16)
        outs[h // per][h % per, PEAK:] = peak
        return None if state_in is None else jnp.exp2((old_peak - peak) * EXPONENT)

    def combine(h, shrink):
        add = jnp.dot(values_ref[:, :count], weights_ref[h % 2, :count, :], preferred_element_type=jnp.float32)[:PEAK]
        if shrink is not None:
            old = state_in[h, :PEAK].reshape(PEAK // 8, 8, rows)
            add = (old * shrink[None]).reshape(PEAK, rows) + add
        outs[h // per][h % per, :PEAK] = add

    top, shrink = {0: score(0)}, {}
    for h in range(heads + 1):
        if h + 1 < heads:
            top[h + 1] = score(h + 1)
        if h >= 1:
            combine(h - 1, shrink[h - 1])
        if h < heads:
            shrink[h] = weigh(h, top[h])


def kernel(head_at, heads, first, n_out, *refs):
    flags, q_ref, kv_ref = refs[:3]
    n = 3
    state_in = None
    if not first:
        state_in = refs[n]
        n += 1
    outs, scratch = refs[n : n + n_out], refs[n + n_out :]
    every = kv_ref.shape[0]

    @pl.when(flags[0] == 0)
    def _():
        for h in range(heads):
            per = heads // n_out
            ref, k = outs[h // per], h % per
            if first:
                ref[k, :PEAK] = jnp.zeros_like(ref[k, :PEAK])
                ref[k, PEAK:] = jnp.full_like(ref[k, PEAK:], EMPTY)
            else:
                ref[k] = state_in[h]

    for n, count in ((1, every // 2), (2, every)):
        pl.when(flags[0] == n)(
            functools.partial(absorb, q_ref, kv_ref, count, flags[1], head_at, heads, state_in, outs, *scratch)
        )


def merge_kernel(mine_ref, theirs_ref, out_ref):
    rows = out_ref.shape[0]
    for h in range(mine_ref.shape[0]):
        peak, peak2 = mine_ref[h, PEAK:], theirs_ref[h, PEAK:]
        top = jnp.maximum(peak, peak2)
        w = jnp.exp2((peak - top) * EXPONENT)
        w2 = jnp.exp2((peak2 - top) * EXPONENT)
        scale = 1.0 / (mine_ref[h, TOTAL:PEAK] * w + theirs_ref[h, TOTAL:PEAK] * w2)
        tiles = (HEAD_DIM // 8, 8, rows)
        normed = mine_ref[h, :HEAD_DIM].reshape(tiles) * (w * scale)[None] + theirs_ref[h, :HEAD_DIM].reshape(
            tiles
        ) * (w2 * scale)[None]
        out_ref[:, h * HEAD_DIM : (h + 1) * HEAD_DIM] = normed.reshape(HEAD_DIM, rows).T.astype(jnp.bfloat16)


VMEM = pl.BlockSpec(memory_space=pltpu.VMEM)
SMEM = pl.BlockSpec(memory_space=pltpu.SMEM)
LIMIT = pltpu.CompilerParams(vmem_limit_bytes=24 * 2**20)


def run(flags, q, kv, state=None, n_out=1, head_at=0):
    rows = q.shape[0]
    heads = GROUP if state is None else state.shape[0]
    keys = kv.shape[0]
    first = state is None
    shape = pltpu.VMEM((heads // n_out, ROWS, rows), jnp.float32)
    return pl.pallas_call(
        functools.partial(kernel, head_at, heads, first, n_out),
        out_shape=shape if n_out == 1 else (shape,) * n_out,
        in_specs=[SMEM] + [VMEM] * (2 + (not first)),
        out_specs=VMEM if n_out == 1 else (VMEM,) * n_out,
        input_output_aliases={} if first or n_out > 1 else {3: 0},
        scratch_shapes=[
            pltpu.VMEM((2, keys, rows), jnp.float32),
            pltpu.VMEM((2, keys, rows), jnp.bfloat16),
            pltpu.VMEM((HEAD_DIM + 16, keys), jnp.bfloat16),
        ],
        cost_estimate=pl.CostEstimate(
            flops=4 * rows * heads * keys * HEAD_DIM,
            bytes_accessed=4 * keys * HEAD_DIM + 2 * rows * heads * HEAD_DIM,
            transcendentals=rows * heads * keys,
        ),
        compiler_params=LIMIT,
    )(flags, q, kv, *(() if first else (state,)))


def spread_kernel(place_ref, keys_ref, values_ref, out_ref):
    both = jnp.concatenate([keys_ref[...], values_ref[...]], 1)
    for n in range(out_ref.shape[0]):
        out_ref[n] = both


def spread(place_of, keys, values, half):
    block = pl.BlockSpec((half, HEAD_DIM), lambda n, at: (at[0], at[1]))
    return pl.pallas_call(
        spread_kernel,
        grid_spec=pltpu.PrefetchScalarGridSpec(
            num_scalar_prefetch=1,
            grid=(1,),
            in_specs=[block, block],
            out_specs=pl.BlockSpec((Y, half, 2 * HEAD_DIM), lambda n, at: (0, 0, 0)),
        ),
        out_shape=jax.ShapeDtypeStruct((Y, half, 2 * HEAD_DIM), jnp.bfloat16),
        compiler_params=LIMIT,
        name="spread",
    )(place_of, *(pltpu.with_memory_space_constraint(a, pltpu.HBM) for a in (keys, values)))


def merge(mine, theirs):
    rows = mine.shape[2]
    return pl.pallas_call(
        merge_kernel,
        out_shape=jax.ShapeDtypeStruct((rows, GROUP // 2 * HEAD_DIM), jnp.bfloat16),
        in_specs=[VMEM] * 2,
        out_specs=VMEM,
        cost_estimate=pl.CostEstimate(flops=rows * HEAD_DIM * 32, bytes_accessed=rows * HEAD_DIM * 32, transcendentals=0),
        compiler_params=LIMIT,
        name="merge",
    )(mine, theirs)


def shards(queries, keys, values):
    ctx, tp = lax.axis_index("ctx"), lax.axis_index("tp")
    y, x, core = ctx // X, ctx % X, tp % C
    rows = queries.shape[0]
    half = rows // 2
    copies = spread(jnp.stack([core, tp // C]).astype(jnp.int32), keys, values, half)
    by_row = lax.all_to_all(
        copies, "ctx", 0, 0, axis_index_groups=[[b * X + a for b in range(Y)] for a in range(X)]
    ).reshape(Y * half, 2 * HEAD_DIM)
    one = move(by_row, 1, -1)
    q = jnp.concatenate([queries, swap(queries)], 1)

    def flags(shift):
        from_x = (x + shift) % X
        delta = (from_x - x - y * X) * rows + core * half
        needed = y + (delta + y * X * rows < rows)
        return jnp.stack([jnp.where(needed == 0, 0, jnp.where(needed <= Y // 2, 1, 2)), delta]).astype(jnp.int32)

    toward = jnp.where(core == 0, -1, 1)
    state = run(flags(0), q, by_row)
    other = move(by_row, -1, 1)
    two = move(one, 1, -1)
    state = run(flags(toward), q, one, state)
    mine, theirs = run(flags(-toward), q, other, state, n_out=2)
    theirs = run(flags(2), q, two, theirs, head_at=GROUP // 2)
    theirs = swap(theirs)
    mine = run(flags(2), q, two, mine)
    return merge(mine, theirs)


def solution(mesh):
    in_specs = (P("ctx", "tp"), P("ctx", None), P("ctx", None))
    return jax.shard_map(shards, mesh=mesh, in_specs=in_specs, out_specs=P("ctx", "tp"), check_vma=False)
```

```python
import functools

import jax
import jax.numpy as jnp
from jax import lax
from jax.experimental import pallas as pl
from jax.experimental.pallas import tpu as pltpu
from jax.sharding import PartitionSpec as P


HEADS = 64
KV_HEADS = 8
HEAD_DIM = 128
GROUP = HEADS // KV_HEADS
Y, X, Z, C = 8, 4, 8, 2
MASKED, EMPTY = -1e30, -1e29
EXPONENT = HEAD_DIM**-0.5 * 1.4426950408889634
TOTAL, PEAK, ROWS = HEAD_DIM, HEAD_DIM + 8, HEAD_DIM + 16


def place(y, x, z, c):
    return (((y % Y) * X + (x % X)) * Z + z) * C + c


def move(a, first, second):
    pairs = [
        (place(y, x, z, c), place(y, x + by, z, c))
        for y in range(Y)
        for x in range(X)
        for z in range(Z)
        for c, by in enumerate((first, second))
    ]
    return lax.ppermute(a, ("ctx", "tp"), pairs)


def swap(a):
    return lax.ppermute(a, "tp", [(i, i ^ 1) for i in range(Z * C)])


def absorb(q_ref, kv_ref, count, delta, head_at, heads, state_in, outs, scores_ref, weights_ref, values_ref):
    rows = q_ref.shape[0]
    half = rows // 2
    values_ref[HEAD_DIM:, :count] = jnp.ones((values_ref.shape[0] - HEAD_DIM, count), jnp.bfloat16)
    for at in range(0, count, rows):
        values_ref[:HEAD_DIM, at : at + rows] = kv_ref[at : at + rows, HEAD_DIM:].T
    ahead = lax.broadcasted_iota(jnp.int32, (half, rows), 0) - lax.broadcasted_iota(jnp.int32, (half, rows), 1)
    per = heads // len(outs)
    first_masked = 0 if count < kv_ref.shape[0] else count // half // 2

    def score(h):
        q = q_ref[:, (head_at + h) * HEAD_DIM : (head_at + h + 1) * HEAD_DIM]
        top = None
        for n in range(count // half):
            at = slice(n * half, (n + 1) * half)
            s = lax.dot_general(
                kv_ref[at, :HEAD_DIM], q, (((1,), (1,)), ((), ())), preferred_element_type=jnp.float32
            )
            if n >= first_masked:
                s = jnp.where(ahead <= -(delta + n * (X * rows)), s, MASKED)
            scores_ref[h % 2, at, :] = s
            t = jnp.max(s.reshape(half // 8, 8, rows), axis=0)
            top = t if top is None else jnp.maximum(top, t)
        return jnp.broadcast_to(jnp.max(top, axis=0, keepdims=True), (8, rows))

    def weigh(h, top):
        old_peak = jnp.full((8, rows), EMPTY, jnp.float32) if state_in is None else state_in[h, PEAK:]
        peak = jnp.maximum(old_peak, top)
        for n in range(count // half):
            at = slice(n * half, (n + 1) * half)
            s = scores_ref[h % 2, at, :].reshape(half // 8, 8, rows)
            w = jnp.exp2((s - peak[None]) * EXPONENT)
            weights_ref[h % 2, at, :] = w.reshape(half, rows).astype(jnp.bfloat16)
        outs[h // per][h % per, PEAK:] = peak
        return None if state_in is None else jnp.exp2((old_peak - peak) * EXPONENT)

    def combine(h, shrink):
        add = jnp.dot(values_ref[:, :count], weights_ref[h % 2, :count, :], preferred_element_type=jnp.float32)[:PEAK]
        if shrink is not None:
            old = state_in[h, :PEAK].reshape(PEAK // 8, 8, rows)
            add = (old * shrink[None]).reshape(PEAK, rows) + add
        outs[h // per][h % per, :PEAK] = add

    top, shrink = {0: score(0)}, {}
    for h in range(heads + 1):
        if h + 1 < heads:
            top[h + 1] = score(h + 1)
        if h >= 1:
            combine(h - 1, shrink[h - 1])
        if h < heads:
            shrink[h] = weigh(h, top[h])


def needs(shift, rows):
    ctx, core = lax.axis_index("ctx"), lax.rem(lax.axis_index("tp"), C)
    y, x = lax.div(ctx, X), lax.rem(ctx, X)
    toward = 2 * core - 1
    from_x = lax.rem(x + shift * (toward if abs(shift) == 1 else 1) + X, X)
    delta = (from_x - x - y * X) * rows + core * (rows // 2)
    needed = y + jnp.where(delta + y * X * rows < rows, 1, 0)
    return jnp.where(needed == 0, 0, jnp.where(needed <= Y // 2, 1, 2)), delta


def kernel(shift, head_at, heads, first, n_out, *refs):
    q_ref, kv_ref = refs[:2]
    n = 2
    amount, delta = needs(shift, q_ref.shape[0])
    state_in = None
    if not first:
        state_in = refs[n]
        n += 1
    outs, scratch = refs[n : n + n_out], refs[n + n_out :]
    every = kv_ref.shape[0]

    @pl.when(amount == 0)
    def _():
        for h in range(heads):
            per = heads // n_out
            ref, k = outs[h // per], h % per
            if first:
                ref[k, :PEAK] = jnp.zeros_like(ref[k, :PEAK])
                ref[k, PEAK:] = jnp.full_like(ref[k, PEAK:], EMPTY)
            else:
                ref[k] = state_in[h]

    for n, count in ((1, every // 2), (2, every)):
        pl.when(amount == n)(
            functools.partial(absorb, q_ref, kv_ref, count, delta, head_at, heads, state_in, outs, *scratch)
        )


def merge_kernel(mine_ref, theirs_ref, out_ref):
    rows = out_ref.shape[0]
    for h in range(mine_ref.shape[0]):
        peak, peak2 = mine_ref[h, PEAK:], theirs_ref[h, PEAK:]
        top = jnp.maximum(peak, peak2)
        w = jnp.exp2((peak - top) * EXPONENT)
        w2 = jnp.exp2((peak2 - top) * EXPONENT)
        scale = 1.0 / (mine_ref[h, TOTAL:PEAK] * w + theirs_ref[h, TOTAL:PEAK] * w2)
        tiles = (HEAD_DIM // 8, 8, rows)
        normed = mine_ref[h, :HEAD_DIM].reshape(tiles) * (w * scale)[None] + theirs_ref[h, :HEAD_DIM].reshape(
            tiles
        ) * (w2 * scale)[None]
        out_ref[:, h * HEAD_DIM : (h + 1) * HEAD_DIM] = normed.reshape(HEAD_DIM, rows).T.astype(jnp.bfloat16)


VMEM = pl.BlockSpec(memory_space=pltpu.VMEM)
LIMIT = pltpu.CompilerParams(vmem_limit_bytes=24 * 2**20)


def run(shift, q, kv, state=None, n_out=1, head_at=0):
    rows = q.shape[0]
    heads = GROUP if state is None else state.shape[0]
    keys = kv.shape[0]
    first = state is None
    shape = pltpu.VMEM((heads // n_out, ROWS, rows), jnp.float32)
    return pl.pallas_call(
        functools.partial(kernel, shift, head_at, heads, first, n_out),
        out_shape=shape if n_out == 1 else (shape,) * n_out,
        in_specs=[VMEM] * (2 + (not first)),
        out_specs=VMEM if n_out == 1 else (VMEM,) * n_out,
        input_output_aliases={} if first or n_out > 1 else {2: 0},
        scratch_shapes=[
            pltpu.VMEM((2, keys, rows), jnp.float32),
            pltpu.VMEM((2, keys, rows), jnp.bfloat16),
            pltpu.VMEM((HEAD_DIM + 16, keys), jnp.bfloat16),
        ],
        cost_estimate=pl.CostEstimate(
            flops=4 * rows * heads * keys * HEAD_DIM,
            bytes_accessed=4 * keys * HEAD_DIM + 2 * rows * heads * HEAD_DIM,
            transcendentals=rows * heads * keys,
        ),
        compiler_params=LIMIT,
    )(q, kv, *(() if first else (state,)))


def spread_kernel(keys_ref, values_ref, out_ref, block_ref, in_sems, out_sems):
    half = block_ref.shape[0]
    tp = lax.axis_index("tp")
    at = pl.ds(pl.multiple_of(lax.rem(tp, C) * half, half), half)
    column = pl.ds(pl.multiple_of(lax.div(tp, C) * HEAD_DIM, HEAD_DIM), HEAD_DIM)
    loads = [
        pltpu.make_async_copy(
            ref.at[at, column], block_ref.at[:, n * HEAD_DIM : (n + 1) * HEAD_DIM], in_sems.at[n]
        )
        for n, ref in enumerate((keys_ref, values_ref))
    ]
    stores = [pltpu.make_async_copy(block_ref, out_ref.at[n], out_sems.at[n]) for n in range(Y)]
    for copy in loads:
        copy.start()
    for copy in loads:
        copy.wait()
    for copy in stores:
        copy.start()
    for copy in stores:
        copy.wait()


def spread(keys, values):
    half = keys.shape[0] // C
    hbm = pl.BlockSpec(memory_space=pltpu.HBM)
    return pl.pallas_call(
        spread_kernel,
        in_specs=[hbm, hbm],
        out_specs=hbm,
        out_shape=jax.ShapeDtypeStruct((Y, half, 2 * HEAD_DIM), jnp.bfloat16),
        scratch_shapes=[
            pltpu.VMEM((half, 2 * HEAD_DIM), jnp.bfloat16),
            pltpu.SemaphoreType.DMA((2,)),
            pltpu.SemaphoreType.DMA((Y,)),
        ],
        compiler_params=LIMIT,
        name="spread",
    )(keys, values)


def merge(mine, theirs):
    rows = mine.shape[2]
    return pl.pallas_call(
        merge_kernel,
        out_shape=jax.ShapeDtypeStruct((rows, GROUP // 2 * HEAD_DIM), jnp.bfloat16),
        in_specs=[VMEM] * 2,
        out_specs=VMEM,
        cost_estimate=pl.CostEstimate(flops=rows * HEAD_DIM * 32, bytes_accessed=rows * HEAD_DIM * 32, transcendentals=0),
        compiler_params=LIMIT,
        name="merge",
    )(mine, theirs)


def shards(queries, keys, values):
    half = queries.shape[0] // C
    copies = spread(keys, values)
    by_row = lax.all_to_all(
        copies, "ctx", 0, 0, axis_index_groups=[[b * X + a for b in range(Y)] for a in range(X)]
    ).reshape(Y * half, 2 * HEAD_DIM)
    one = move(by_row, 1, -1)
    q = jnp.concatenate([queries, swap(queries)], 1)
    state = run(0, q, by_row)
    other = move(by_row, -1, 1)
    two = move(one, 1, -1)
    state = run(1, q, one, state)
    mine, theirs = run(-1, q, other, state, n_out=2)
    theirs = run(2, q, two, theirs, head_at=GROUP // 2)
    theirs = swap(theirs)
    mine = run(2, q, two, mine)
    return merge(mine, theirs)


def solution(mesh):
    in_specs = (P("ctx", "tp"), P("ctx", None), P("ctx", None))
    return jax.shard_map(shards, mesh=mesh, in_specs=in_specs, out_specs=P("ctx", "tp"), check_vma=False)
```

```python
import functools

import jax
import jax.numpy as jnp
from jax import lax
from jax.experimental import pallas as pl
from jax.experimental.pallas import tpu as pltpu
from jax.sharding import PartitionSpec as P


HEADS = 64
KV_HEADS = 8
HEAD_DIM = 128
GROUP = HEADS // KV_HEADS
Y, X, Z, C = 8, 4, 8, 2
MASKED, EMPTY = -1e30, -1e29
EXPONENT = HEAD_DIM**-0.5 * 1.4426950408889634
TOTAL, PEAK, ROWS = HEAD_DIM, HEAD_DIM + 8, HEAD_DIM + 16


def place(y, x, z, c):
    return (((y % Y) * X + (x % X)) * Z + z) * C + c


def move(a, first, second):
    pairs = [
        (place(y, x, z, c), place(y, x + by, z, c))
        for y in range(Y)
        for x in range(X)
        for z in range(Z)
        for c, by in enumerate((first, second))
    ]
    return lax.ppermute(a, ("ctx", "tp"), pairs)


def swap(a):
    return lax.ppermute(a, "tp", [(i, i ^ 1) for i in range(Z * C)])


def absorb(q_ref, kv_refs, count, delta, masks, head_at, heads, state_in, outs, scores_ref, weights_ref, values_ref):
    rows = q_ref.shape[0]
    sub = rows // C
    size = kv_refs[0].shape[0]
    parts = [
        (kv_refs[at // size], at % size, at // sub * (X * rows), masks[0] <= at < masks[1])
        for at in range(0, count, sub)
    ]
    total = len(parts) * sub
    values_ref[HEAD_DIM:, :total] = jnp.ones((values_ref.shape[0] - HEAD_DIM, total), jnp.bfloat16)
    for n, (ref, at, _, _) in enumerate(parts):
        values_ref[:HEAD_DIM, n * sub : (n + 1) * sub] = ref[at : at + sub, HEAD_DIM:].T
    ahead = lax.broadcasted_iota(jnp.int32, (sub, rows), 0) - lax.broadcasted_iota(jnp.int32, (sub, rows), 1)
    per = heads // len(outs)

    def score(h):
        q = q_ref[:, (head_at + h) * HEAD_DIM : (head_at + h + 1) * HEAD_DIM]
        top = None
        for n, (ref, at, place_of, masked) in enumerate(parts):
            s = lax.dot_general(
                ref[at : at + sub, :HEAD_DIM], q, (((1,), (1,)), ((), ())), preferred_element_type=jnp.float32
            )
            if masked:
                s = jnp.where(ahead <= -(delta + place_of), s, MASKED)
            scores_ref[h % 2, n * sub : (n + 1) * sub, :] = s
            t = jnp.max(s.reshape(sub // 8, 8, rows), axis=0)
            top = t if top is None else jnp.maximum(top, t)
        return jnp.broadcast_to(jnp.max(top, axis=0, keepdims=True), (8, rows))

    def weigh(h, top):
        old_peak = jnp.full((8, rows), EMPTY, jnp.float32) if state_in is None else state_in[h, PEAK:]
        peak = jnp.maximum(old_peak, top)
        for n in range(len(parts)):
            at = slice(n * sub, (n + 1) * sub)
            s = scores_ref[h % 2, at, :].reshape(sub // 8, 8, rows)
            w = jnp.exp2((s - peak[None]) * EXPONENT)
            weights_ref[h % 2, at, :] = w.reshape(sub, rows).astype(jnp.bfloat16)
        outs[h // per][h % per, PEAK:] = peak
        return None if state_in is None else jnp.exp2((old_peak - peak) * EXPONENT)

    def combine(h, shrink):
        add = jnp.dot(values_ref[:, :total], weights_ref[h % 2, :total, :], preferred_element_type=jnp.float32)[:PEAK]
        if shrink is not None:
            old = state_in[h, :PEAK].reshape(PEAK // 8, 8, rows)
            add = (old * shrink[None]).reshape(PEAK, rows) + add
        outs[h // per][h % per, :PEAK] = add

    top, shrink = {0: score(0)}, {}
    for h in range(heads + 1):
        if h + 1 < heads:
            top[h + 1] = score(h + 1)
        if h >= 1:
            combine(h - 1, shrink[h - 1])
        if h < heads:
            shrink[h] = weigh(h, top[h])


def needs(shift, rows):
    ctx, core = lax.axis_index("ctx"), lax.rem(lax.axis_index("tp"), C)
    y, x = lax.div(ctx, X), lax.rem(ctx, X)
    toward = 2 * core - 1
    from_x = lax.rem(x + shift * (toward if abs(shift) == 1 else 1) + X, X)
    delta = (from_x - x - y * X) * rows + core * (rows // 2)
    needed = y + jnp.where(delta + y * X * rows < rows, 1, 0)
    return jnp.where(needed == 0, 0, jnp.where(needed <= Y // 2, 1, 2)), delta


def kernel(shift, n_kv, head_at, heads, first, n_out, *refs):
    q_ref, kv_refs = refs[0], refs[1 : 1 + n_kv]
    n = 1 + n_kv
    amount, delta = needs(shift, q_ref.shape[0])
    every = sum(ref.shape[0] for ref in kv_refs)
    state_in = None
    if not first:
        state_in = refs[n]
        n += 1
    outs, scratch = refs[n : n + n_out], refs[n + n_out :]

    @pl.when(amount == 0)
    def _():
        for h in range(heads):
            per = heads // n_out
            ref, k = outs[h // per], h % per
            if first:
                ref[k, :PEAK] = jnp.zeros_like(ref[k, :PEAK])
                ref[k, PEAK:] = jnp.full_like(ref[k, PEAK:], EMPTY)
            else:
                ref[k] = state_in[h]

    for n, count, masks in ((1, every // 2, (0, every)), (2, every, (every // 2, every))):
        pl.when(amount == n)(
            functools.partial(
                absorb, q_ref, kv_refs, count, delta, masks, head_at, heads, state_in, outs, *scratch
            )
        )


def merge_kernel(mine_ref, theirs_ref, out_ref):
    rows = out_ref.shape[0]
    for h in range(mine_ref.shape[0]):
        peak, peak2 = mine_ref[h, PEAK:], theirs_ref[h, PEAK:]
        top = jnp.maximum(peak, peak2)
        w = jnp.exp2((peak - top) * EXPONENT)
        w2 = jnp.exp2((peak2 - top) * EXPONENT)
        scale = 1.0 / (mine_ref[h, TOTAL:PEAK] * w + theirs_ref[h, TOTAL:PEAK] * w2)
        tiles = (HEAD_DIM // 8, 8, rows)
        normed = mine_ref[h, :HEAD_DIM].reshape(tiles) * (w * scale)[None] + theirs_ref[h, :HEAD_DIM].reshape(
            tiles
        ) * (w2 * scale)[None]
        out_ref[:, h * HEAD_DIM : (h + 1) * HEAD_DIM] = normed.reshape(HEAD_DIM, rows).T.astype(jnp.bfloat16)


VMEM = pl.BlockSpec(memory_space=pltpu.VMEM)
LIMIT = pltpu.CompilerParams(vmem_limit_bytes=24 * 2**20)


def run(shift, q, kvs, state=None, n_out=1, head_at=0):
    rows = q.shape[0]
    heads = GROUP if state is None else state.shape[0]
    keys = sum(kv.shape[0] for kv in kvs)
    first = state is None
    shape = pltpu.VMEM((heads // n_out, ROWS, rows), jnp.float32)
    return pl.pallas_call(
        functools.partial(kernel, shift, len(kvs), head_at, heads, first, n_out),
        out_shape=shape if n_out == 1 else (shape,) * n_out,
        in_specs=[VMEM] * (1 + len(kvs) + (not first)),
        out_specs=VMEM if n_out == 1 else (VMEM,) * n_out,
        input_output_aliases={} if first or n_out > 1 else {1 + len(kvs): 0},
        scratch_shapes=[
            pltpu.VMEM((2, keys, rows), jnp.float32),
            pltpu.VMEM((2, keys, rows), jnp.bfloat16),
            pltpu.VMEM((HEAD_DIM + 16, keys), jnp.bfloat16),
        ],
        cost_estimate=pl.CostEstimate(
            flops=4 * rows * heads * keys * HEAD_DIM,
            bytes_accessed=4 * keys * HEAD_DIM + 2 * rows * heads * HEAD_DIM,
            transcendentals=rows * heads * keys,
        ),
        compiler_params=LIMIT,
    )(q, *kvs, *(() if first else (state,)))


def spread_kernel(keys_ref, values_ref, out_ref, block_ref, in_sems, out_sems):
    half = block_ref.shape[0]
    tp = lax.axis_index("tp")
    at = pl.ds(pl.multiple_of(lax.rem(tp, C) * half, half), half)
    column = pl.ds(pl.multiple_of(lax.div(tp, C) * HEAD_DIM, HEAD_DIM), HEAD_DIM)
    loads = [
        pltpu.make_async_copy(
            ref.at[at, column], block_ref.at[:, n * HEAD_DIM : (n + 1) * HEAD_DIM], in_sems.at[n]
        )
        for n, ref in enumerate((keys_ref, values_ref))
    ]
    stores = [pltpu.make_async_copy(block_ref, out_ref.at[n], out_sems.at[n]) for n in range(Y)]
    for copy in loads:
        copy.start()
    for copy in loads:
        copy.wait()
    for copy in stores:
        copy.start()
    for copy in stores:
        copy.wait()


def spread(keys, values):
    half = keys.shape[0] // C
    hbm = pl.BlockSpec(memory_space=pltpu.HBM)
    return pl.pallas_call(
        spread_kernel,
        in_specs=[hbm, hbm],
        out_specs=hbm,
        out_shape=jax.ShapeDtypeStruct((Y, half, 2 * HEAD_DIM), jnp.bfloat16),
        scratch_shapes=[
            pltpu.VMEM((half, 2 * HEAD_DIM), jnp.bfloat16),
            pltpu.SemaphoreType.DMA((2,)),
            pltpu.SemaphoreType.DMA((Y,)),
        ],
        compiler_params=LIMIT,
        name="spread",
    )(*(pltpu.with_memory_space_constraint(a, pltpu.HBM) for a in (keys, values)))


def merge(mine, theirs):
    rows = mine.shape[2]
    return pl.pallas_call(
        merge_kernel,
        out_shape=jax.ShapeDtypeStruct((rows, GROUP // 2 * HEAD_DIM), jnp.bfloat16),
        in_specs=[VMEM] * 2,
        out_specs=VMEM,
        cost_estimate=pl.CostEstimate(flops=rows * HEAD_DIM * 32, bytes_accessed=rows * HEAD_DIM * 32, transcendentals=0),
        compiler_params=LIMIT,
        name="merge",
    )(mine, theirs)


def shards(queries, keys, values):
    groups = [[b * X + a for b in range(Y)] for a in range(X)]
    own = lax.all_to_all(spread(keys, values), "ctx", 0, 0, axis_index_groups=groups).reshape(-1, 2 * HEAD_DIM)
    q = jnp.concatenate([queries, swap(queries)], 1)
    near = []
    for rows in jnp.split(own, 2):
        near.append(move(rows, 1, -1))
    other = move(own, -1, 1)
    far = []
    for chunk in near:
        far.append(move(chunk, 1, -1))
    state = run(0, q, [own])
    state = run(1, q, near, state)
    mine, theirs = run(-1, q, [other], state, n_out=2)
    theirs = run(2, q, far, theirs, head_at=GROUP // 2)
    theirs = swap(theirs)
    mine = run(2, q, far, mine)
    return merge(mine, theirs)


def solution(mesh):
    in_specs = (P("ctx", "tp"), P("ctx", None), P("ctx", None))
    return jax.shard_map(shards, mesh=mesh, in_specs=in_specs, out_specs=P("ctx", "tp"), check_vma=False)
```

```python
import functools

import jax
import jax.numpy as jnp
from jax import lax
from jax.experimental import pallas as pl
from jax.experimental.pallas import tpu as pltpu
from jax.sharding import PartitionSpec as P


HEADS = 64
KV_HEADS = 8
HEAD_DIM = 128
GROUP = HEADS // KV_HEADS
Y, X, Z, C = 8, 4, 8, 2
MASKED, EMPTY = -1e30, -1e29
EXPONENT = HEAD_DIM**-0.5 * 1.4426950408889634
TOTAL, PEAK, ROWS = HEAD_DIM, HEAD_DIM + 8, HEAD_DIM + 16


def place(y, x, z, c):
    return (((y % Y) * X + (x % X)) * Z + z) * C + c


def move(a, first, second, start=0):
    pairs = [
        (place(y, x, z, c), place(y, x + by, z, c))
        for y in range(start, Y)
        for x in range(X)
        for z in range(Z)
        for c, by in enumerate((first, second))
    ]
    return lax.ppermute(a, ("ctx", "tp"), pairs)


def swap(a):
    return lax.ppermute(a, "tp", [(i, i ^ 1) for i in range(Z * C)])


def absorb(q_ref, kv_refs, count, delta, masks, head_at, heads, state_in, outs, scores_ref, weights_ref, values_ref):
    rows = q_ref.shape[0]
    sub = rows // C
    size = kv_refs[0].shape[0]
    parts = [
        (kv_refs[at // size], at % size, at // sub * (X * rows), masks[0] <= at < masks[1])
        for at in range(0, count, sub)
    ]
    total = len(parts) * sub
    values_ref[HEAD_DIM:, :total] = jnp.ones((values_ref.shape[0] - HEAD_DIM, total), jnp.bfloat16)
    for n, (ref, at, _, _) in enumerate(parts):
        values_ref[:HEAD_DIM, n * sub : (n + 1) * sub] = ref[at : at + sub, HEAD_DIM:].T
    ahead = lax.broadcasted_iota(jnp.int32, (sub, rows), 0) - lax.broadcasted_iota(jnp.int32, (sub, rows), 1)
    per = heads // len(outs)

    def score(h):
        q = q_ref[:, (head_at + h) * HEAD_DIM : (head_at + h + 1) * HEAD_DIM]
        top = None
        for n, (ref, at, place_of, masked) in enumerate(parts):
            s = lax.dot_general(
                ref[at : at + sub, :HEAD_DIM], q, (((1,), (1,)), ((), ())), preferred_element_type=jnp.float32
            )
            if masked:
                s = jnp.where(ahead <= -(delta + place_of), s, MASKED)
            scores_ref[h % 2, n * sub : (n + 1) * sub, :] = s
            t = jnp.max(s.reshape(sub // 8, 8, rows), axis=0)
            top = t if top is None else jnp.maximum(top, t)
        return jnp.broadcast_to(jnp.max(top, axis=0, keepdims=True), (8, rows))

    def weigh(h, top):
        old_peak = jnp.full((8, rows), EMPTY, jnp.float32) if state_in is None else state_in[h, PEAK:]
        peak = jnp.maximum(old_peak, top)
        for n in range(len(parts)):
            at = slice(n * sub, (n + 1) * sub)
            s = scores_ref[h % 2, at, :].reshape(sub // 8, 8, rows)
            w = jnp.exp2((s - peak[None]) * EXPONENT)
            weights_ref[h % 2, at, :] = w.reshape(sub, rows).astype(jnp.bfloat16)
        outs[h // per][h % per, PEAK:] = peak
        return None if state_in is None else jnp.exp2((old_peak - peak) * EXPONENT)

    def combine(h, shrink):
        add = jnp.dot(values_ref[:, :total], weights_ref[h % 2, :total, :], preferred_element_type=jnp.float32)[:PEAK]
        if shrink is not None:
            old = state_in[h, :PEAK].reshape(PEAK // 8, 8, rows)
            add = (old * shrink[None]).reshape(PEAK, rows) + add
        outs[h // per][h % per, :PEAK] = add

    top, shrink = {0: score(0)}, {}
    for h in range(heads + 1):
        if h + 1 < heads:
            top[h + 1] = score(h + 1)
        if h >= 1:
            combine(h - 1, shrink[h - 1])
        if h < heads:
            shrink[h] = weigh(h, top[h])


def needs(shift, rows):
    ctx, core = lax.axis_index("ctx"), lax.rem(lax.axis_index("tp"), C)
    y, x = lax.div(ctx, X), lax.rem(ctx, X)
    toward = 2 * core - 1
    from_x = lax.rem(x + shift * (toward if abs(shift) == 1 else 1) + X, X)
    delta = (from_x - x - y * X) * rows + core * (rows // 2)
    needed = y + jnp.where(delta + y * X * rows < rows, 1, 0)
    return jnp.where(needed == 0, 0, jnp.where(needed <= Y // 2, 1, 2)), delta


def kernel(shift, n_kv, head_at, heads, first, n_out, *refs):
    q_ref, kv_refs = refs[0], refs[1 : 1 + n_kv]
    n = 1 + n_kv
    amount, delta = needs(shift, q_ref.shape[0])
    every = sum(ref.shape[0] for ref in kv_refs)
    state_in = None
    if not first:
        state_in = refs[n]
        n += 1
    outs, scratch = refs[n : n + n_out], refs[n + n_out :]

    @pl.when(amount == 0)
    def _():
        for h in range(heads):
            per = heads // n_out
            ref, k = outs[h // per], h % per
            if first:
                ref[k, :PEAK] = jnp.zeros_like(ref[k, :PEAK])
                ref[k, PEAK:] = jnp.full_like(ref[k, PEAK:], EMPTY)
            else:
                ref[k] = state_in[h]

    for n, count, masks in ((1, every // 2, (0, every)), (2, every, (every // 2, every))):
        pl.when(amount == n)(
            functools.partial(
                absorb, q_ref, kv_refs, count, delta, masks, head_at, heads, state_in, outs, *scratch
            )
        )


def merge_kernel(mine_ref, theirs_ref, out_ref):
    rows = out_ref.shape[0]
    for h in range(mine_ref.shape[0]):
        peak, peak2 = mine_ref[h, PEAK:], theirs_ref[h, PEAK:]
        top = jnp.maximum(peak, peak2)
        w = jnp.exp2((peak - top) * EXPONENT)
        w2 = jnp.exp2((peak2 - top) * EXPONENT)
        scale = 1.0 / (mine_ref[h, TOTAL:PEAK] * w + theirs_ref[h, TOTAL:PEAK] * w2)
        tiles = (HEAD_DIM // 8, 8, rows)
        normed = mine_ref[h, :HEAD_DIM].reshape(tiles) * (w * scale)[None] + theirs_ref[h, :HEAD_DIM].reshape(
            tiles
        ) * (w2 * scale)[None]
        out_ref[:, h * HEAD_DIM : (h + 1) * HEAD_DIM] = normed.reshape(HEAD_DIM, rows).T.astype(jnp.bfloat16)


VMEM = pl.BlockSpec(memory_space=pltpu.VMEM)
LIMIT = pltpu.CompilerParams(vmem_limit_bytes=24 * 2**20)


def run(shift, q, kvs, state=None, n_out=1, head_at=0):
    rows = q.shape[0]
    heads = GROUP if state is None else state.shape[0]
    keys = sum(kv.shape[0] for kv in kvs)
    first = state is None
    shape = pltpu.VMEM((heads // n_out, ROWS, rows), jnp.float32)
    return pl.pallas_call(
        functools.partial(kernel, shift, len(kvs), head_at, heads, first, n_out),
        out_shape=shape if n_out == 1 else (shape,) * n_out,
        in_specs=[VMEM] * (1 + len(kvs) + (not first)),
        out_specs=VMEM if n_out == 1 else (VMEM,) * n_out,
        input_output_aliases={} if first or n_out > 1 else {1 + len(kvs): 0},
        scratch_shapes=[
            pltpu.VMEM((2, keys, rows), jnp.float32),
            pltpu.VMEM((2, keys, rows), jnp.bfloat16),
            pltpu.VMEM((HEAD_DIM + 16, keys), jnp.bfloat16),
        ],
        cost_estimate=pl.CostEstimate(
            flops=4 * rows * heads * keys * HEAD_DIM,
            bytes_accessed=4 * keys * HEAD_DIM + 2 * rows * heads * HEAD_DIM,
            transcendentals=rows * heads * keys,
        ),
        compiler_params=LIMIT,
    )(q, *kvs, *(() if first else (state,)))


def spread_kernel(keys_ref, values_ref, out_ref, block_ref, in_sems, out_sems):
    half = block_ref.shape[0]
    tp = lax.axis_index("tp")
    at = pl.ds(pl.multiple_of(lax.rem(tp, C) * half, half), half)
    column = pl.ds(pl.multiple_of(lax.div(tp, C) * HEAD_DIM, HEAD_DIM), HEAD_DIM)
    loads = [
        pltpu.make_async_copy(
            ref.at[at, column], block_ref.at[:, n * HEAD_DIM : (n + 1) * HEAD_DIM], in_sems.at[n]
        )
        for n, ref in enumerate((keys_ref, values_ref))
    ]
    stores = [pltpu.make_async_copy(block_ref, out_ref.at[n], out_sems.at[n]) for n in range(Y)]
    for copy in loads:
        copy.start()
    for copy in loads:
        copy.wait()
    for copy in stores:
        copy.start()
    for copy in stores:
        copy.wait()


def spread(keys, values):
    half = keys.shape[0] // C
    hbm = pl.BlockSpec(memory_space=pltpu.HBM)
    return pl.pallas_call(
        spread_kernel,
        in_specs=[hbm, hbm],
        out_specs=hbm,
        out_shape=jax.ShapeDtypeStruct((Y, half, 2 * HEAD_DIM), jnp.bfloat16),
        scratch_shapes=[
            pltpu.VMEM((half, 2 * HEAD_DIM), jnp.bfloat16),
            pltpu.SemaphoreType.DMA((2,)),
            pltpu.SemaphoreType.DMA((Y,)),
        ],
        compiler_params=LIMIT,
        name="spread",
    )(*(pltpu.with_memory_space_constraint(a, pltpu.HBM) for a in (keys, values)))


def merge(mine, theirs):
    rows = mine.shape[2]
    return pl.pallas_call(
        merge_kernel,
        out_shape=jax.ShapeDtypeStruct((rows, GROUP // 2 * HEAD_DIM), jnp.bfloat16),
        in_specs=[VMEM] * 2,
        out_specs=VMEM,
        cost_estimate=pl.CostEstimate(flops=rows * HEAD_DIM * 32, bytes_accessed=rows * HEAD_DIM * 32, transcendentals=0),
        compiler_params=LIMIT,
        name="merge",
    )(mine, theirs)


def shards(queries, keys, values):
    groups = [[b * X + a for b in range(Y)] for a in range(X)]
    own = lax.all_to_all(spread(keys, values), "ctx", 0, 0, axis_index_groups=groups).reshape(-1, 2 * HEAD_DIM)
    q = jnp.concatenate([queries, swap(queries)], 1)
    near = []
    for n, rows in enumerate(jnp.split(own, 2)):
        near.append(move(rows, 1, -1, n * (Y // 2)))
    other = move(own, -1, 1)
    far = []
    for n, chunk in enumerate(near):
        far.append(move(chunk, 1, -1, n * (Y // 2)))
    state = run(0, q, [own])
    state = run(1, q, near, state)
    mine, theirs = run(-1, q, [other], state, n_out=2)
    theirs = run(2, q, far, theirs, head_at=GROUP // 2)
    theirs = swap(theirs)
    mine = run(2, q, far, mine)
    return merge(mine, theirs)


def solution(mesh):
    in_specs = (P("ctx", "tp"), P("ctx", None), P("ctx", None))
    return jax.shard_map(shards, mesh=mesh, in_specs=in_specs, out_specs=P("ctx", "tp"), check_vma=False)
```

```python
import functools

import jax
import jax.numpy as jnp
from jax import lax
from jax.experimental import pallas as pl
from jax.experimental.pallas import tpu as pltpu
from jax.sharding import PartitionSpec as P


HEADS = 64
KV_HEADS = 8
HEAD_DIM = 128
GROUP = HEADS // KV_HEADS
Y, X, Z, C = 8, 4, 8, 2
STEPS = (4, 6, 8)
MASKED, EMPTY = -1e30, -1e29
EXPONENT = HEAD_DIM**-0.5 * 1.4426950408889634
TOTAL, PEAK, ROWS = HEAD_DIM, HEAD_DIM + 8, HEAD_DIM + 16


def place(y, x, z, c):
    return (((y % Y) * X + (x % X)) * Z + z) * C + c


def move(a, first, second, start=0):
    pairs = [
        (place(y, x, z, c), place(y, x + by, z, c))
        for y in range(start, Y)
        for x in range(X)
        for z in range(Z)
        for c, by in enumerate((first, second))
    ]
    return lax.ppermute(a, ("ctx", "tp"), pairs)


def swap(a):
    return lax.ppermute(a, "tp", [(i, i ^ 1) for i in range(Z * C)])


def absorb(q_ref, kv_refs, from_row, count, delta, masks, head_at, heads, state_in, outs, scores_ref, weights_ref, values_ref):
    rows = q_ref.shape[0]
    sub = rows // C
    size = kv_refs[0].shape[0]
    parts = [
        (kv_refs[at // size], at % size, (from_row + at // sub) * (X * rows), at >= masks)
        for at in range(0, count, sub)
    ]
    total = len(parts) * sub
    values_ref[HEAD_DIM:, :total] = jnp.ones((values_ref.shape[0] - HEAD_DIM, total), jnp.bfloat16)
    for n, (ref, at, _, _) in enumerate(parts):
        values_ref[:HEAD_DIM, n * sub : (n + 1) * sub] = ref[at : at + sub, HEAD_DIM:].T
    ahead = lax.broadcasted_iota(jnp.int32, (sub, rows), 0) - lax.broadcasted_iota(jnp.int32, (sub, rows), 1)
    per = heads // len(outs)

    def score(h):
        q = q_ref[:, (head_at + h) * HEAD_DIM : (head_at + h + 1) * HEAD_DIM]
        top = None
        for n, (ref, at, place_of, masked) in enumerate(parts):
            s = lax.dot_general(
                ref[at : at + sub, :HEAD_DIM], q, (((1,), (1,)), ((), ())), preferred_element_type=jnp.float32
            )
            if masked:
                s = jnp.where(ahead <= -(delta + place_of), s, MASKED)
            scores_ref[h % 2, n * sub : (n + 1) * sub, :] = s
            t = jnp.max(s.reshape(sub // 8, 8, rows), axis=0)
            top = t if top is None else jnp.maximum(top, t)
        return jnp.broadcast_to(jnp.max(top, axis=0, keepdims=True), (8, rows))

    def weigh(h, top):
        old_peak = jnp.full((8, rows), EMPTY, jnp.float32) if state_in is None else state_in[h, PEAK:]
        peak = jnp.maximum(old_peak, top)
        for n in range(len(parts)):
            at = slice(n * sub, (n + 1) * sub)
            s = scores_ref[h % 2, at, :].reshape(sub // 8, 8, rows)
            w = jnp.exp2((s - peak[None]) * EXPONENT)
            weights_ref[h % 2, at, :] = w.reshape(sub, rows).astype(jnp.bfloat16)
        outs[h // per][h % per, PEAK:] = peak
        return None if state_in is None else jnp.exp2((old_peak - peak) * EXPONENT)

    def combine(h, shrink):
        add = jnp.dot(values_ref[:, :total], weights_ref[h % 2, :total, :], preferred_element_type=jnp.float32)[:PEAK]
        if shrink is not None:
            old = state_in[h, :PEAK].reshape(PEAK // 8, 8, rows)
            add = (old * shrink[None]).reshape(PEAK, rows) + add
        outs[h // per][h % per, :PEAK] = add

    top, shrink = {0: score(0)}, {}
    for h in range(heads + 1):
        if h + 1 < heads:
            top[h + 1] = score(h + 1)
        if h >= 1:
            combine(h - 1, shrink[h - 1])
        if h < heads:
            shrink[h] = weigh(h, top[h])


def needs(shift, rows):
    ctx, core = lax.axis_index("ctx"), lax.rem(lax.axis_index("tp"), C)
    y, x = lax.div(ctx, X), lax.rem(ctx, X)
    toward = 2 * core - 1
    from_x = lax.rem(x + shift * (toward if abs(shift) == 1 else 1) + X, X)
    delta = (from_x - x - y * X) * rows + core * (rows // 2)
    needed = y + jnp.where(delta + y * X * rows < rows, 1, 0)
    amount = sum(jnp.where(needed > n, 1, 0) for n in (0,) + STEPS[:-1])
    return amount, delta


def kernel(shift, n_kv, from_row, head_at, heads, first, n_out, *refs):
    q_ref, kv_refs = refs[0], refs[1 : 1 + n_kv]
    n = 1 + n_kv
    amount, delta = needs(shift, q_ref.shape[0])
    every = sum(ref.shape[0] for ref in kv_refs)
    state_in = None
    if not first:
        state_in = refs[n]
        n += 1
    outs, scratch = refs[n : n + n_out], refs[n + n_out :]

    def keep():
        for h in range(heads):
            per = heads // n_out
            ref, k = outs[h // per], h % per
            if first:
                ref[k, :PEAK] = jnp.zeros_like(ref[k, :PEAK])
                ref[k, PEAK:] = jnp.full_like(ref[k, PEAK:], EMPTY)
            else:
                ref[k] = state_in[h]

    sub = q_ref.shape[0] // C
    for n, needed in enumerate((0,) + STEPS):
        count = min((needed - from_row) * sub, every)
        masks = (STEPS[n - 2] - from_row) * sub if n > 1 else 0
        act = keep
        if count > 0:
            act = functools.partial(
                absorb, q_ref, kv_refs, from_row, count, delta, masks, head_at, heads, state_in, outs, *scratch
            )
        pl.when(amount == n)(act)


def merge_kernel(mine_ref, theirs_ref, out_ref):
    rows = out_ref.shape[0]
    for h in range(mine_ref.shape[0]):
        peak, peak2 = mine_ref[h, PEAK:], theirs_ref[h, PEAK:]
        top = jnp.maximum(peak, peak2)
        w = jnp.exp2((peak - top) * EXPONENT)
        w2 = jnp.exp2((peak2 - top) * EXPONENT)
        scale = 1.0 / (mine_ref[h, TOTAL:PEAK] * w + theirs_ref[h, TOTAL:PEAK] * w2)
        tiles = (HEAD_DIM // 8, 8, rows)
        normed = mine_ref[h, :HEAD_DIM].reshape(tiles) * (w * scale)[None] + theirs_ref[h, :HEAD_DIM].reshape(
            tiles
        ) * (w2 * scale)[None]
        out_ref[:, h * HEAD_DIM : (h + 1) * HEAD_DIM] = normed.reshape(HEAD_DIM, rows).astype(jnp.bfloat16).T


VMEM = pl.BlockSpec(memory_space=pltpu.VMEM)
LIMIT = pltpu.CompilerParams(vmem_limit_bytes=24 * 2**20)


def run(shift, q, kvs, state=None, n_out=1, head_at=0, from_row=0):
    rows = q.shape[0]
    heads = GROUP if state is None else state.shape[0]
    keys = sum(kv.shape[0] for kv in kvs)
    first = state is None
    shape = pltpu.VMEM((heads // n_out, ROWS, rows), jnp.float32)
    return pl.pallas_call(
        functools.partial(kernel, shift, len(kvs), from_row, head_at, heads, first, n_out),
        out_shape=shape if n_out == 1 else (shape,) * n_out,
        in_specs=[VMEM] * (1 + len(kvs) + (not first)),
        out_specs=VMEM if n_out == 1 else (VMEM,) * n_out,
        input_output_aliases={} if first or n_out > 1 else {1 + len(kvs): 0},
        scratch_shapes=[
            pltpu.VMEM((2, keys, rows), jnp.float32),
            pltpu.VMEM((2, keys, rows), jnp.bfloat16),
            pltpu.VMEM((HEAD_DIM + 16, keys), jnp.bfloat16),
        ],
        cost_estimate=pl.CostEstimate(
            flops=4 * rows * heads * keys * HEAD_DIM,
            bytes_accessed=4 * keys * HEAD_DIM + 2 * rows * heads * HEAD_DIM,
            transcendentals=rows * heads * keys,
        ),
        compiler_params=LIMIT,
    )(q, *kvs, *(() if first else (state,)))


def spread_kernel(keys_ref, values_ref, out_ref, block_ref, in_sems, out_sems):
    half = block_ref.shape[0]
    tp = lax.axis_index("tp")
    at = pl.ds(pl.multiple_of(lax.rem(tp, C) * half, half), half)
    column = pl.ds(pl.multiple_of(lax.div(tp, C) * HEAD_DIM, HEAD_DIM), HEAD_DIM)
    loads = [
        pltpu.make_async_copy(
            ref.at[at, column], block_ref.at[:, n * HEAD_DIM : (n + 1) * HEAD_DIM], in_sems.at[n]
        )
        for n, ref in enumerate((keys_ref, values_ref))
    ]
    stores = [pltpu.make_async_copy(block_ref, out_ref.at[n], out_sems.at[n]) for n in range(Y)]
    for copy in loads:
        copy.start()
    for copy in loads:
        copy.wait()
    for copy in stores:
        copy.start()
    for copy in stores:
        copy.wait()


def spread(keys, values):
    half = keys.shape[0] // C
    hbm = pl.BlockSpec(memory_space=pltpu.HBM)
    return pl.pallas_call(
        spread_kernel,
        in_specs=[hbm, hbm],
        out_specs=hbm,
        out_shape=jax.ShapeDtypeStruct((Y, half, 2 * HEAD_DIM), jnp.bfloat16),
        scratch_shapes=[
            pltpu.VMEM((half, 2 * HEAD_DIM), jnp.bfloat16),
            pltpu.SemaphoreType.DMA((2,)),
            pltpu.SemaphoreType.DMA((Y,)),
        ],
        compiler_params=LIMIT,
        name="spread",
    )(*(pltpu.with_memory_space_constraint(a, pltpu.HBM) for a in (keys, values)))


def merge(mine, theirs):
    rows = mine.shape[2]
    return pl.pallas_call(
        merge_kernel,
        out_shape=jax.ShapeDtypeStruct((rows, GROUP // 2 * HEAD_DIM), jnp.bfloat16),
        in_specs=[VMEM] * 2,
        out_specs=VMEM,
        cost_estimate=pl.CostEstimate(flops=rows * HEAD_DIM * 32, bytes_accessed=rows * HEAD_DIM * 32, transcendentals=0),
        compiler_params=LIMIT,
        name="merge",
    )(mine, theirs)


def shards(queries, keys, values):
    groups = [[b * X + a for b in range(Y)] for a in range(X)]
    own = lax.all_to_all(spread(keys, values), "ctx", 0, 0, axis_index_groups=groups).reshape(-1, 2 * HEAD_DIM)
    q = jnp.concatenate([queries, swap(queries)], 1)
    near = []
    for n, rows in enumerate(jnp.split(own, 2)):
        near.append(move(rows, 1, -1, n * (Y // 2)))
    other = move(own, -1, 1)
    far = []
    for n, chunk in enumerate(near):
        far.append(move(chunk, 1, -1, n * (Y // 2)))
    state = run(0, q, [own])
    state = run(1, q, near, state)
    state = run(-1, q, [other], state)
    mine, theirs = run(2, q, far[:1], state, n_out=2)
    theirs = run(2, q, far[1:], theirs, head_at=GROUP // 2, from_row=Y // 2)
    theirs = swap(theirs)
    mine = run(2, q, far[1:], mine, from_row=Y // 2)
    return merge(mine, theirs)


def solution(mesh):
    in_specs = (P("ctx", "tp"), P("ctx", None), P("ctx", None))
    return jax.shard_map(shards, mesh=mesh, in_specs=in_specs, out_specs=P("ctx", "tp"), check_vma=False)
```

```python
import functools

import jax
import jax.numpy as jnp
from jax import lax
from jax.experimental import pallas as pl
from jax.experimental.pallas import tpu as pltpu
from jax.sharding import PartitionSpec as P


HEADS = 64
KV_HEADS = 8
HEAD_DIM = 128
GROUP = HEADS // KV_HEADS
Y, X, Z, C = 8, 4, 8, 2
STEPS = (4, 6, 8)
MASKED, EMPTY = -1e30, -1e29
EXPONENT = HEAD_DIM**-0.5 * 1.4426950408889634
TOTAL, PEAK, ROWS = HEAD_DIM, HEAD_DIM + 8, HEAD_DIM + 16


def place(y, x, z, c):
    return (((y % Y) * X + (x % X)) * Z + z) * C + c


def move(a, first, second, start=0):
    pairs = [
        (place(y, x, z, c), place(y, x + by, z, c))
        for y in range(start, Y)
        for x in range(X)
        for z in range(Z)
        for c, by in enumerate((first, second))
    ]
    return lax.ppermute(a, ("ctx", "tp"), pairs)


def swap(a):
    return lax.ppermute(a, "tp", [(i, i ^ 1) for i in range(Z * C)])


def absorb(q_ref, kv_refs, count, delta, masks, head_at, heads, state_in, outs, scores_ref, weights_ref, values_ref):
    rows = q_ref.shape[0]
    sub = rows // C
    size = kv_refs[0].shape[0]
    parts = [
        (kv_refs[at // size], at % size, at // sub * (X * rows), masks[0] <= at < masks[1])
        for at in range(0, count, sub)
    ]
    total = len(parts) * sub
    values_ref[HEAD_DIM:, :total] = jnp.ones((values_ref.shape[0] - HEAD_DIM, total), jnp.bfloat16)
    for n, (ref, at, _, _) in enumerate(parts):
        values_ref[:HEAD_DIM, n * sub : (n + 1) * sub] = ref[at : at + sub, HEAD_DIM:].T
    ahead = lax.broadcasted_iota(jnp.int32, (sub, rows), 0) - lax.broadcasted_iota(jnp.int32, (sub, rows), 1)
    per = heads // len(outs)

    def score(h):
        q = q_ref[:, (head_at + h) * HEAD_DIM : (head_at + h + 1) * HEAD_DIM]
        top = None
        for n, (ref, at, place_of, masked) in enumerate(parts):
            s = lax.dot_general(
                ref[at : at + sub, :HEAD_DIM], q, (((1,), (1,)), ((), ())), preferred_element_type=jnp.float32
            )
            if masked:
                s = jnp.where(ahead <= -(delta + place_of), s, MASKED)
            scores_ref[h % 2, n * sub : (n + 1) * sub, :] = s
            t = jnp.max(s.reshape(sub // 8, 8, rows), axis=0)
            top = t if top is None else jnp.maximum(top, t)
        return jnp.broadcast_to(jnp.max(top, axis=0, keepdims=True), (8, rows))

    def weigh(h, top):
        old_peak = jnp.full((8, rows), EMPTY, jnp.float32) if state_in is None else state_in[h, PEAK:]
        peak = jnp.maximum(old_peak, top)
        for n in range(len(parts)):
            at = slice(n * sub, (n + 1) * sub)
            s = scores_ref[h % 2, at, :].reshape(sub // 8, 8, rows)
            w = jnp.exp2((s - peak[None]) * EXPONENT)
            weights_ref[h % 2, at, :] = w.reshape(sub, rows).astype(jnp.bfloat16)
        outs[h // per][h % per, PEAK:] = peak
        return None if state_in is None else jnp.exp2((old_peak - peak) * EXPONENT)

    def combine(h, shrink):
        add = jnp.dot(values_ref[:, :total], weights_ref[h % 2, :total, :], preferred_element_type=jnp.float32)[:PEAK]
        if shrink is not None:
            old = state_in[h, :PEAK].reshape(PEAK // 8, 8, rows)
            add = (old * shrink[None]).reshape(PEAK, rows) + add
        outs[h // per][h % per, :PEAK] = add

    top, shrink = {0: score(0)}, {}
    for h in range(heads + 1):
        if h + 1 < heads:
            top[h + 1] = score(h + 1)
        if h >= 1:
            combine(h - 1, shrink[h - 1])
        if h < heads:
            shrink[h] = weigh(h, top[h])


def needs(shift, rows):
    ctx, core = lax.axis_index("ctx"), lax.rem(lax.axis_index("tp"), C)
    y, x = lax.div(ctx, X), lax.rem(ctx, X)
    toward = 2 * core - 1
    from_x = lax.rem(x + shift * (toward if abs(shift) == 1 else 1) + X, X)
    delta = (from_x - x - y * X) * rows + core * (rows // 2)
    needed = y + jnp.where(delta + y * X * rows < rows, 1, 0)
    amount = sum(jnp.where(needed > n, 1, 0) for n in (0,) + STEPS[:-1])
    return amount, delta


def kernel(shift, n_kv, head_at, heads, first, n_out, *refs):
    q_ref, kv_refs = refs[0], refs[1 : 1 + n_kv]
    n = 1 + n_kv
    amount, delta = needs(shift, q_ref.shape[0])
    every = sum(ref.shape[0] for ref in kv_refs)
    state_in = None
    if not first:
        state_in = refs[n]
        n += 1
    outs, scratch = refs[n : n + n_out], refs[n + n_out :]

    @pl.when(amount == 0)
    def _():
        for h in range(heads):
            per = heads // n_out
            ref, k = outs[h // per], h % per
            if first:
                ref[k, :PEAK] = jnp.zeros_like(ref[k, :PEAK])
                ref[k, PEAK:] = jnp.full_like(ref[k, PEAK:], EMPTY)
            else:
                ref[k] = state_in[h]

    for n, last in enumerate(STEPS):
        first_masked = STEPS[n - 1] if n else 0
        count, masks = every // Y * last, (every // Y * first_masked, every)
        pl.when(amount == n + 1)(
            functools.partial(
                absorb, q_ref, kv_refs, count, delta, masks, head_at, heads, state_in, outs, *scratch
            )
        )


def merge_kernel(mine_ref, theirs_ref, out_ref):
    rows = out_ref.shape[0]
    for h in range(mine_ref.shape[0]):
        peak, peak2 = mine_ref[h, PEAK:], theirs_ref[h, PEAK:]
        top = jnp.maximum(peak, peak2)
        w = jnp.exp2((peak - top) * EXPONENT)
        w2 = jnp.exp2((peak2 - top) * EXPONENT)
        scale = 1.0 / (mine_ref[h, TOTAL:PEAK] * w + theirs_ref[h, TOTAL:PEAK] * w2)
        tiles = (HEAD_DIM // 8, 8, rows)
        normed = mine_ref[h, :HEAD_DIM].reshape(tiles) * (w * scale)[None] + theirs_ref[h, :HEAD_DIM].reshape(
            tiles
        ) * (w2 * scale)[None]
        out_ref[:, h * HEAD_DIM : (h + 1) * HEAD_DIM] = normed.reshape(HEAD_DIM, rows).astype(jnp.bfloat16).T


VMEM = pl.BlockSpec(memory_space=pltpu.VMEM)
LIMIT = pltpu.CompilerParams(vmem_limit_bytes=24 * 2**20)
SPREAD_OUT = pltpu.CompilerParams(vmem_limit_bytes=24 * 2**20)


def run(shift, q, kvs, state=None, n_out=1, head_at=0):
    rows = q.shape[0]
    heads = GROUP if state is None else state.shape[0]
    keys = sum(kv.shape[0] for kv in kvs)
    first = state is None
    shape = pltpu.VMEM((heads // n_out, ROWS, rows), jnp.float32)
    return pl.pallas_call(
        functools.partial(kernel, shift, len(kvs), head_at, heads, first, n_out),
        out_shape=shape if n_out == 1 else (shape,) * n_out,
        in_specs=[VMEM] * (1 + len(kvs) + (not first)),
        out_specs=VMEM if n_out == 1 else (VMEM,) * n_out,
        input_output_aliases={} if first or n_out > 1 else {1 + len(kvs): 0},
        scratch_shapes=[
            pltpu.VMEM((2, keys, rows), jnp.float32),
            pltpu.VMEM((2, keys, rows), jnp.bfloat16),
            pltpu.VMEM((HEAD_DIM + 16, keys), jnp.bfloat16),
        ],
        cost_estimate=pl.CostEstimate(
            flops=4 * rows * heads * keys * HEAD_DIM,
            bytes_accessed=4 * keys * HEAD_DIM + 2 * rows * heads * HEAD_DIM,
            transcendentals=rows * heads * keys,
        ),
        compiler_params=SPREAD_OUT,
    )(q, *kvs, *(() if first else (state,)))


def spread_kernel(keys_ref, values_ref, out_ref, block_ref, in_sems, out_sems):
    half = block_ref.shape[0]
    tp = lax.axis_index("tp")
    at = pl.ds(pl.multiple_of(lax.rem(tp, C) * half, half), half)
    column = pl.ds(pl.multiple_of(lax.div(tp, C) * HEAD_DIM, HEAD_DIM), HEAD_DIM)
    loads = [
        pltpu.make_async_copy(
            ref.at[at, column], block_ref.at[:, n * HEAD_DIM : (n + 1) * HEAD_DIM], in_sems.at[n]
        )
        for n, ref in enumerate((keys_ref, values_ref))
    ]
    stores = [pltpu.make_async_copy(block_ref, out_ref.at[n], out_sems.at[n]) for n in range(Y)]
    for copy in loads:
        copy.start()
    for copy in loads:
        copy.wait()
    for copy in stores:
        copy.start()
    for copy in stores:
        copy.wait()


def spread(keys, values):
    half = keys.shape[0] // C
    hbm = pl.BlockSpec(memory_space=pltpu.HBM)
    return pl.pallas_call(
        spread_kernel,
        in_specs=[hbm, hbm],
        out_specs=hbm,
        out_shape=jax.ShapeDtypeStruct((Y, half, 2 * HEAD_DIM), jnp.bfloat16),
        scratch_shapes=[
            pltpu.VMEM((half, 2 * HEAD_DIM), jnp.bfloat16),
            pltpu.SemaphoreType.DMA((2,)),
            pltpu.SemaphoreType.DMA((Y,)),
        ],
        compiler_params=LIMIT,
        name="spread",
    )(*(pltpu.with_memory_space_constraint(a, pltpu.HBM) for a in (keys, values)))


def merge(mine, theirs):
    rows = mine.shape[2]
    return pl.pallas_call(
        merge_kernel,
        out_shape=jax.ShapeDtypeStruct((rows, GROUP // 2 * HEAD_DIM), jnp.bfloat16),
        in_specs=[VMEM] * 2,
        out_specs=VMEM,
        cost_estimate=pl.CostEstimate(flops=rows * HEAD_DIM * 32, bytes_accessed=rows * HEAD_DIM * 32, transcendentals=0),
        compiler_params=LIMIT,
        name="merge",
    )(mine, theirs)


def shards(queries, keys, values):
    groups = [[b * X + a for b in range(Y)] for a in range(X)]
    own = lax.all_to_all(spread(keys, values), "ctx", 0, 0, axis_index_groups=groups).reshape(-1, 2 * HEAD_DIM)
    q = jnp.concatenate([queries, swap(queries)], 1)
    near = []
    for n, rows in enumerate(jnp.split(own, 2)):
        near.append(move(rows, 1, -1, n * (Y // 2)))
    other = move(own, -1, 1)
    far = []
    for n, chunk in enumerate(near):
        far.append(move(chunk, 1, -1, n * (Y // 2)))
    state = run(0, q, [own])
    state = run(1, q, near, state)
    mine, theirs = run(-1, q, [other], state, n_out=2)
    theirs = run(2, q, far, theirs, head_at=GROUP // 2)
    theirs = swap(theirs)
    mine = run(2, q, far, mine)
    return merge(mine, theirs)


def solution(mesh):
    in_specs = (P("ctx", "tp"), P("ctx", None), P("ctx", None))
    return jax.shard_map(shards, mesh=mesh, in_specs=in_specs, out_specs=P("ctx", "tp"), check_vma=False)
```
